256 devices in a mesh: mol: 16 (over x_lo, y, core), grid: 16 (over x_hi, z).
Axes of the slice: x: 4 (x_hi: 2, x_lo: 2; x = x_hi * 2 + x_lo), y: 4, z: 8, core: 2. Of those that a mesh axis runs over, the one named last changes fastest.
Arguments:
- cells_start: int32 [131072], P('mol'), may hold values from 0 to 2097151
- moves: int32 [2, 3, 131072], P(None, None, 'mol'), may hold values from -1 to 1
- accepted: int32 [2, 131072], P(None, 'mol'), may hold values from 0 to 1
- bead_types: int32 [131072], P('mol'), may hold values from 0 to 1
Outputs:
- energy_change: float32 [2, 131072], P(None, 'mol')
- final_field: bfloat16 [64, 64, 1024], P('mol', 'grid')
The draws below stay inside these ranges and needn't reach their ends.
All inputs are finite; a program needn't handle non-finite values.
Results may differ from the reference program's by a relative error of at most 0.0048.
Values may be sent and summed in bfloat16 or wider, within the bound.
No kernel may reach another device: no remote copies, remote signals or barrier semaphores. Data moves between devices by JAX's collectives and lax.ppermute only.
A program may use at most 64 MiB of HBM per device.

```python
import jax
import jax.numpy as jnp

NX = 512
NY = 64
STEPS = 2
TYPES = 2
SPREAD = 2
NZ = 64
BEADS = 131072
CELLS = 2097152


def place_ends(array, rng, least, largest):
    spot = [jax.random.randint(jax.random.fold_in(rng, axis), (), 0, length) for axis, length in enumerate(array.shape)]
    longest = array.shape.index(max(array.shape))
    beside = spot[:longest] + [(spot[longest] + 1) % array.shape[longest]] + spot[longest + 1:]
    return array.at[tuple(spot)].set(least).at[tuple(beside)].set(largest)


def setup_inputs(seed: int = 0) -> dict:
    keys = jax.random.split(jax.random.key(seed), 5)
    cells_start = place_ends(jax.random.randint(keys[0], (BEADS,), 0, CELLS), jax.random.fold_in(keys[0], 1), 0, CELLS - 1).astype(jnp.int32)
    moves = place_ends(jax.random.randint(keys[1], (STEPS, 3, BEADS), -1, 2), jax.random.fold_in(keys[1], 1), -1, 1).astype(jnp.int32)
    accepted = place_ends(jax.random.randint(keys[2], (STEPS, BEADS), 0, 2), jax.random.fold_in(keys[2], 1), 0, 1).astype(jnp.int32)
    bead_types = place_ends(jax.random.randint(keys[3], (BEADS,), 0, TYPES), jax.random.fold_in(keys[3], 1), 0, TYPES - 1).astype(jnp.int32)
    return dict(cells_start=cells_start, moves=moves, accepted=accepted, bead_types=bead_types)


chi_mix = 1.0
kappa_comp = 0.5


def kernel_table():
    column = jnp.arange(NX, dtype=jnp.float32)
    distance = jnp.abs(column[:, None] - column[None, :])
    distance = jnp.minimum(distance, NX - distance)
    weights = jnp.exp(-distance * distance / (2.0 * SPREAD * SPREAD))
    first = jnp.abs(column)
    first = jnp.minimum(first, NX - first)
    total = jnp.sum(jnp.exp(-first * first / (2.0 * SPREAD * SPREAD)))
    return (weights / total).astype(jnp.bfloat16)


def split_cell(cells):
    col_x = cells % NX
    row_y = (cells // NX) % NY
    plane_z = cells // (NX * NY)
    return col_x, row_y, plane_z


def move_cells(cells, shift):
    col_x, row_y, plane_z = split_cell(cells)
    col_x = (col_x + shift[0]) % NX
    row_y = (row_y + shift[1]) % NY
    plane_z = (plane_z + shift[2]) % NZ
    return ((plane_z * NY + row_y) * NX + col_x).astype(jnp.int32)


def deposit(positions, bead_types, kernel):
    col_x, row_y, plane_z = split_cell(positions)
    rows = kernel[col_x].astype(jnp.float32)
    first = jnp.where(bead_types[:, None] == 0, rows, 0.0)
    second = jnp.where(bead_types[:, None] == 1, rows, 0.0)
    spread_rows = jnp.concatenate([first, second], axis=1)
    segment = (row_y * NZ + plane_z).astype(jnp.int32)
    summed = jax.ops.segment_sum(spread_rows, segment, num_segments=NY * NZ)
    scale = NX * NY * NZ / BEADS
    return (scale * summed).reshape(NY, NZ, 2 * NX)


def make_field(density):
    phi_a = density[:, :, :NX]
    phi_b = density[:, :, NX:]
    excess = kappa_comp * (phi_a + phi_b - 1.0)
    field_a = chi_mix * phi_b + excess
    field_b = chi_mix * phi_a + excess
    return jnp.concatenate([field_a, field_b], axis=2).astype(jnp.bfloat16)


def read_field(field, cells, bead_types):
    col_x, row_y, plane_z = split_cell(cells)
    flat_index = ((row_y * NZ + plane_z) * 2 + bead_types) * NX + col_x
    return jnp.take(field.reshape(-1), flat_index.astype(jnp.int32)).astype(jnp.float32)


def reference(cells_start, moves, accepted, bead_types):
    kernel = kernel_table()
    positions = cells_start
    changes = []
    field = None
    for step in range(STEPS):
        proposed = move_cells(positions, moves[step])
        field = make_field(deposit(positions, bead_types, kernel))
        changes.append(read_field(field, proposed, bead_types) - read_field(field, positions, bead_types))
        positions = jnp.where(accepted[step] == 1, proposed, positions)
    return jnp.stack(changes), field
```

```python
import functools

import jax
import jax.numpy as jnp
from jax import lax
from jax.experimental import pallas as pl
from jax.experimental.pallas import tpu as pltpu
from jax.sharding import PartitionSpec as P

NX = 512
NY = 64
ZDEV = 4
STEPS = 2
SPREAD = 2
GROUPS = 16
SLOTS = 128
CHUNK = 256
SETS = 4
MSG = 80
F32 = jnp.float32
BF16 = jnp.bfloat16
CONTRACT_LANES = (((1,), (1,)), ((), ()))
CONTRACT_SUBLANES = (((0,), (0,)), ((), ()))


chi_mix = 1.0
kappa_comp = 0.5


def split_up(x, dim, size):
    shape = x.shape
    blocks = x.reshape(*shape[:dim], size, shape[dim] // size, *shape[dim + 1 :])
    return jnp.moveaxis(blocks, dim, 0)


def sum_at_owner(x, axis, dim):
    blocks = split_up(x, dim, lax.axis_size(axis))
    arrived = lax.all_to_all(blocks, axis, split_axis=0, concat_axis=0, tiled=True)
    return arrived.sum(axis=0)


def laid_out(blocks, dim):
    blocks = jnp.moveaxis(blocks, 0, dim)
    shape = blocks.shape
    return blocks.reshape(*shape[:dim], shape[dim] * shape[dim + 1], *shape[dim + 2 :])


def sent_to_all(x, axis):
    copies = jnp.broadcast_to(x, (lax.axis_size(axis), *x.shape))
    return lax.all_to_all(copies, axis, split_axis=0, concat_axis=0, tiled=True)


def collect(x, axis, dim):
    return laid_out(sent_to_all(x, axis), dim)


def of_everyone(x, axis):
    return sent_to_all(x, axis).astype(jnp.float32).sum(axis=0)


def kernel_rows(col_x):
    column = jnp.arange(NX, dtype=jnp.float32)
    distance = jnp.abs(column[None, :] - col_x.astype(jnp.float32)[:, None])
    distance = jnp.minimum(distance, NX - distance)
    weights = jnp.exp(-distance * distance / (2.0 * SPREAD * SPREAD))
    first = jnp.abs(column)
    first = jnp.minimum(first, NX - first)
    total = jnp.sum(jnp.exp(-first * first / (2.0 * SPREAD * SPREAD)))
    return (weights / total).astype(jnp.bfloat16)


def split_cell(cells):
    col_x = cells % NX
    row_y = cells // NX % NY
    plane_z = cells // (NX * NY)
    return (col_x, row_y, plane_z)


def move_cells(cells, shift, planes):
    col_x, row_y, plane_z = split_cell(cells)
    col_x = (col_x + shift[0]) % NX
    row_y = (row_y + shift[1]) % NY
    plane_z = (plane_z + shift[2]) % planes
    return (plane_z * NY + row_y) * NX + col_x


def deposit(positions, bead_types, slab, start, count):
    col_x, row_y, plane_z = split_cell(positions)
    inside = (plane_z // ZDEV == slab) & (row_y >= start) & (row_y < start + count)
    row_id = jnp.where(inside, row_y * ZDEV + plane_z - slab * ZDEV, -1)
    bead_count = positions.shape[0]
    block_size = min(1024, bead_count)
    row_total = count * ZDEV
    targets = lax.broadcasted_iota(jnp.int32, (row_total, block_size), 0)

    def add_block(block_id, total):
        begin = block_id * block_size
        rows_here = lax.dynamic_slice_in_dim(row_id, begin, block_size)
        cols_here = lax.dynamic_slice_in_dim(col_x, begin, block_size)
        types_here = lax.dynamic_slice_in_dim(bead_types, begin, block_size)
        onehot = (rows_here[None, :] == targets).astype(jnp.bfloat16)
        spread_rows = kernel_rows(cols_here)
        zeros_bf = jnp.zeros_like(spread_rows)
        first = jnp.where(types_here[:, None] == 0, spread_rows, zeros_bf)
        second = jnp.where(types_here[:, None] == 1, spread_rows, zeros_bf)
        columns = jnp.concatenate([first, second], axis=1)
        return total + jnp.dot(onehot, columns, preferred_element_type=jnp.float32)

    empty = jnp.zeros((row_total, 2 * NX), jnp.float32)
    total = lax.fori_loop(0, bead_count // block_size, add_block, empty)
    return total.reshape(count, ZDEV, 2 * NX)


def make_field(density):
    phi_a = density[:, :, :NX]
    phi_b = density[:, :, NX:]
    excess = kappa_comp * (phi_a + phi_b - 1.0)
    field_a = chi_mix * phi_b + excess
    field_b = chi_mix * phi_a + excess
    return jnp.concatenate([field_a, field_b], axis=2).astype(jnp.bfloat16)


def make_reader(points, bead_types, z_first, z_span):
    col_x, row_y, plane_z = split_cell(points)
    local_z = plane_z - z_first
    kinds = jnp.broadcast_to(bead_types[None, :], points.shape)
    column_id = kinds * NX + col_x

    def read_beads(carry, piece, start):
        span_rows = piece.shape[0]
        flat_table = piece.reshape(-1)
        valid = (row_y >= 0) & (row_y < span_rows) & (local_z >= 0) & (local_z < z_span)
        flat_index = jnp.where(valid, (row_y * z_span + local_z) * (2 * NX) + column_id, 0)
        picked = jnp.take(flat_table, flat_index).astype(jnp.float32)
        return jnp.where(valid, picked, 0.0)

    return read_beads


def any_spread(cells_start, moves, accepted, bead_types):
    grid_count = lax.axis_size("grid")
    mol_count = lax.axis_size("mol")
    slab = lax.axis_index("grid")
    planes = ZDEV * grid_count
    bead_count = cells_start.shape[0]
    scale = NX * NY * planes / (bead_count * mol_count)
    band_rows = NY // mol_count
    positions = [cells_start]
    proposals = []
    for step in range(STEPS):
        proposed = move_cells(positions[step], moves[step], planes)
        proposals.append(proposed)
        positions.append(jnp.where(accepted[step] == 1, proposed, positions[step]))
    fields = []
    for step in range(STEPS):

        def step_term(start, count, current=positions[step]):
            return deposit(current, bead_types, slab, start, count)

        summed = sum_at_owner(step_term(jnp.int32(0), band_rows * lax.axis_size("mol")), "mol", 0)
        fields.append(make_field(scale * summed))
    changes = []
    for step in range(STEPS):
        points = jnp.stack([positions[step], proposals[step]])
        start_values = jnp.zeros(points.shape, jnp.float32)
        reader = make_reader(points, bead_types, slab * ZDEV, ZDEV)
        partial_values = reader(start_values, collect(fields[step], "mol", 0), jnp.int32(0))
        values = of_everyone(partial_values.astype(jnp.bfloat16), "grid").astype(jnp.float32)
        changes.append(values[1] - values[0])
    return (jnp.stack(changes), fields[STEPS - 1])


def one_hot(row, count, base=0):
    width = row.shape[1]
    tile = jnp.broadcast_to(row, (16, width)).astype(BF16)
    iota = lax.broadcasted_iota(jnp.int32, (16, width), 0).astype(F32)
    one = jnp.ones((16, width), BF16)
    zero = jnp.zeros((16, width), BF16)
    parts = [
        jnp.where(tile == (iota + float(base + first)).astype(BF16), one, zero)
        for first in range(0, count, 16)
    ]
    return jnp.concatenate(parts, axis=0) if len(parts) > 1 else parts[0]


def bucket_kernel(slab_ref, cells_ref, moves_ref, accepted_ref, types_ref, msg_ref, own_ref, slot_ref,
                  code, cls, dig_h, dig_l, one_y, one_s, ranked, prefix, left, right):
    beads = cells_ref.shape[1]
    chunks = beads // CHUNK
    slab = slab_ref[0]
    kind = types_ref[...] << 21

    def moved(cell, step):
        col_x = (cell + moves_ref[step, 0:1, :]) & (NX - 1)
        row_y = ((cell >> 9) + moves_ref[step, 1:2, :]) & (NY - 1)
        plane = ((cell >> 15) + moves_ref[step, 2:3, :]) & (ZDEV * GROUPS - 1)
        return col_x | (row_y << 9) | (plane << 15)

    start = cells_ref[...]
    first = moved(start, 0)
    after = jnp.where(accepted_ref[0:1, :] == 1, first, start)
    second = moved(after, 1)
    code[0:1, :] = start | kind
    code[1:2, :] = after | kind
    code[2:3, :] = first | kind
    code[3:4, :] = second | kind
    c = code[...]
    block_y = (c >> 11) & 15
    block_z = (c >> 17) & 15
    row = ((c >> 9) & 3) * 4 + ((c >> 15) & 3)
    high = ((c >> 7) & 3) * 32 + (c >> 21) * 16 + row
    cls[0:SETS, :] = block_y.astype(F32)
    cls[SETS : 2 * SETS, :] = block_z.astype(F32)
    dig_h[...] = (high + 1).astype(F32)
    dig_l[...] = (c & 127).astype(F32)
    inside_all = jnp.where(block_z == slab, 1.0, 0.0)
    cls[2 * SETS : 3 * SETS, :] = inside_all
    for s in range(SETS):
        y_hot = one_hot(cls[s : s + 1, :], 16)
        one_y[s * 16 : s * 16 + 16, :] = y_hot
        one_s[s * 16 : s * 16 + 16, :] = one_hot(cls[SETS + s : SETS + s + 1, :], 16)
        inside = jnp.broadcast_to(cls[2 * SETS + s : 2 * SETS + s + 1, :], (16, beads)).astype(BF16)
        mask = y_hot * inside
        left[s * 32 : s * 32 + 16, :] = mask * jnp.broadcast_to(dig_h[s : s + 1, :], (16, beads)).astype(BF16)
        left[s * 32 + 16 : s * 32 + 32, :] = mask * jnp.broadcast_to(dig_l[s : s + 1, :], (16, beads)).astype(BF16)
        for k in range(chunks):
            at = (s * chunks + k) * 16
            ranked[at : at + 16, :] = mask[:, k * CHUNK : (k + 1) * CHUNK]
    counts = lax.dot_general(one_s[...], one_y[...], CONTRACT_LANES, preferred_element_type=F32)
    same = (
        lax.broadcasted_iota(jnp.int32, counts.shape, 0) // 16
        == lax.broadcasted_iota(jnp.int32, counts.shape, 1) // 16
    )
    largest = jnp.max(jnp.where(same, counts, 0.0))
    over = jnp.where(largest > float(SLOTS), 1.0, 0.0)
    rows = lax.broadcasted_iota(jnp.int32, (CHUNK, CHUNK + 128), 0)
    cols = lax.broadcasted_iota(jnp.int32, (CHUNK, CHUNK + 128), 1)
    upto = jnp.where((rows <= cols) | (cols >= CHUNK), 1.0, 0.0).astype(BF16)
    prefix[...] = jnp.dot(ranked[...], upto, preferred_element_type=F32)
    for s in range(SETS):
        carry = jnp.zeros((16, 128), F32)
        for k in range(chunks):
            at = (s * chunks + k) * 16
            mine = ranked[at : at + 16, :].astype(F32)
            ahead = prefix[at : at + 16, 0:CHUNK] + jnp.concatenate([carry, carry], axis=1)
            rank = jnp.sum(mine * ahead, axis=0, keepdims=True) - 1.0
            carry = carry + prefix[at : at + 16, CHUNK : CHUNK + 128]
            lanes = slice(k * CHUNK, (k + 1) * CHUNK)
            right[:, lanes] = one_hot(rank, SLOTS)
            slot_ref[s : s + 1, lanes] = jnp.where(rank >= 0.0, cls[s : s + 1, lanes] * SLOTS + rank, -1.0).astype(jnp.int32)
        own_ref[s * 32 : s * 32 + 32, :] = lax.dot_general(
            left[s * 32 : s * 32 + 32, :], right[...], CONTRACT_LANES, preferred_element_type=F32
        ).astype(BF16)
    for j in range(GROUPS):
        msg_ref[j, 0:64, :] = own_ref[0:64, :]
        msg_ref[j, 64:MSG, :] = jnp.broadcast_to(over, (MSG - 64, SLOTS)).astype(BF16)


def bucket(slab, cells, moves, accepted, types):
    beads = cells.shape[0]
    vmem = pl.BlockSpec(memory_space=pltpu.VMEM)
    return pl.pallas_call(
        bucket_kernel,
        out_shape=(
            jax.ShapeDtypeStruct((GROUPS, MSG, SLOTS), BF16),
            jax.ShapeDtypeStruct((SETS * 32, SLOTS), BF16),
            jax.ShapeDtypeStruct((SETS, beads), jnp.int32),
        ),
        in_specs=[pl.BlockSpec(memory_space=pltpu.SMEM)] + [vmem] * 4,
        out_specs=(vmem, vmem, vmem),
        scratch_shapes=[
            pltpu.VMEM((SETS, beads), jnp.int32),
            pltpu.VMEM((3 * SETS, beads), F32),
            pltpu.VMEM((SETS, beads), F32),
            pltpu.VMEM((SETS, beads), F32),
            pltpu.VMEM((SETS * 16, beads), BF16),
            pltpu.VMEM((SETS * 16, beads), BF16),
            pltpu.VMEM((SETS * beads // CHUNK * 16, CHUNK), BF16),
            pltpu.VMEM((SETS * beads // CHUNK * 16, CHUNK + 128), F32),
            pltpu.VMEM((SETS * 32, beads), BF16),
            pltpu.VMEM((SLOTS, beads), BF16),
        ],
        name="bucket",
    )(slab, cells.reshape(1, beads), moves, accepted, types.reshape(1, beads))


def field_kernel(scale, place_ref, msg_ref, own_ref, slot_ref, table_ref, field_ref, change_ref,
                 hot_h, hot_l, count_lo, count_hi, field, values):
    def count_block(step, block):
        for j in range(GROUPS):
            lanes = slice(j * SLOTS, (j + 1) * SLOTS)
            hot_h[:, lanes] = one_hot(msg_ref[j, pl.ds(step * 32 + block, 1), :].astype(F32), 128, 1)
            hot_l[:, lanes] = one_hot(msg_ref[j, pl.ds(step * 32 + 16 + block, 1), :].astype(F32), 128)
        hist = lax.dot_general(hot_h[...], hot_l[...], CONTRACT_LANES, preferred_element_type=F32)
        high = jnp.floor(hist * (1.0 / 256.0))
        low = hist - 256.0 * high
        at = pl.multiple_of((step * GROUPS + block) * 32, 32)
        for q in range(4):
            count_lo[pl.ds(at, 32), q * 128 : (q + 1) * 128] = low[q * 32 : (q + 1) * 32, :].astype(BF16)
            count_hi[pl.ds(at, 32), q * 128 : (q + 1) * 128] = high[q * 32 : (q + 1) * 32, :].astype(BF16)

    for step in range(STEPS):
        for block in range(GROUPS):
            count_block(step, block)
    table = table_ref[...]
    for step in range(STEPS):
        at = step * GROUPS * 32
        rows = GROUPS * 32
        dens = jnp.dot(count_lo[at : at + rows, :], table, preferred_element_type=F32)
        dens += 256.0 * jnp.dot(count_hi[at : at + rows, :], table, preferred_element_type=F32)
        dens = dens * scale
        for block in range(GROUPS):
            phi_a = dens[block * 32 : block * 32 + 16, :]
            phi_b = dens[block * 32 + 16 : block * 32 + 32, :]
            excess = kappa_comp * (phi_a + phi_b - 1.0)
            field[at + block * 32 : at + block * 32 + 16, :] = (chi_mix * phi_b + excess).astype(BF16)
            field[at + block * 32 + 16 : at + block * 32 + 32, :] = (chi_mix * phi_a + excess).astype(BF16)
    mine = pl.multiple_of(((STEPS - 1) * GROUPS + place_ref[0]) * 32, 32)
    field_ref[:, 0:NX] = field[pl.ds(mine, 16), :]
    field_ref[:, NX : 2 * NX] = field[pl.ds(mine + 16, 16), :]
    for step in range(STEPS):
        for block in range(GROUPS):
            at = (step * GROUPS + block) * 32
            cells = jnp.concatenate([field[at : at + 32, q * 128 : (q + 1) * 128] for q in range(4)], axis=0)
            hots, lows = [], []
            for s in (step, STEPS + step):
                hots.append(one_hot(own_ref[s * 32 + block : s * 32 + block + 1, :].astype(F32), 128, 1))
                low = jnp.broadcast_to(own_ref[s * 32 + 16 + block : s * 32 + 17 + block, :].astype(F32), (128, SLOTS))
                lows.append(low)
            picked = lax.dot_general(
                cells, jnp.concatenate(hots, axis=1), CONTRACT_SUBLANES, preferred_element_type=F32
            )
            lanes = lax.broadcasted_iota(jnp.int32, (128, 2 * SLOTS), 0).astype(F32)
            chosen = jnp.where(jnp.concatenate(lows, axis=1) == lanes, picked, 0.0)
            got = jnp.sum(chosen, axis=0, keepdims=True)
            values[step * 32 + block : step * 32 + block + 1, :] = got[:, 0:SLOTS]
            values[step * 32 + 16 + block : step * 32 + 17 + block, :] = got[:, SLOTS:]
    for step in range(STEPS):
        back = []
        for which in range(2):
            slot = slot_ref[which * STEPS + step]
            rank = slot & (SLOTS - 1)
            home = slot >> 7
            total = jnp.zeros(slot.shape, F32)
            for block in range(GROUPS):
                at = step * 32 + which * 16 + block
                line = jnp.broadcast_to(values[at : at + 1, :], slot.shape)
                total = jnp.where(home == block, jnp.take_along_axis(line, rank, axis=1), total)
            back.append(total)
        change = (back[1] - back[0]).astype(BF16)
        for j in range(GROUPS):
            change_ref[j, step] = change


def fields_and_changes(scale, place, msg, own, slot, table):
    rows = slot.shape[1]
    vmem = pl.BlockSpec(memory_space=pltpu.VMEM)
    return pl.pallas_call(
        functools.partial(field_kernel, scale),
        out_shape=(
            jax.ShapeDtypeStruct((16, 2 * NX), BF16),
            jax.ShapeDtypeStruct((GROUPS, STEPS, rows, 128), BF16),
        ),
        in_specs=[pl.BlockSpec(memory_space=pltpu.SMEM)] + [vmem] * 4,
        out_specs=(vmem, vmem),
        scratch_shapes=[
            pltpu.VMEM((128, GROUPS * SLOTS), BF16),
            pltpu.VMEM((128, GROUPS * SLOTS), BF16),
            pltpu.VMEM((STEPS * GROUPS * 32, NX), BF16),
            pltpu.VMEM((STEPS * GROUPS * 32, NX), BF16),
            pltpu.VMEM((STEPS * GROUPS * 32, NX), BF16),
            pltpu.VMEM((STEPS * 32, SLOTS), F32),
        ],
        name="fields",
    )(place, msg, own, slot, table)


def local(cells_start, moves, accepted, bead_types):
    beads = cells_start.shape[0]
    slab = lax.axis_index("grid").astype(jnp.int32).reshape(1)
    place = lax.axis_index("mol").astype(jnp.int32).reshape(1)
    scale = NX * NY * ZDEV * GROUPS / (beads * GROUPS)
    msg, own, slot = bucket(slab, cells_start, moves, accepted, bead_types)
    msg = lax.all_to_all(msg, "mol", split_axis=0, concat_axis=0, tiled=True)
    crowded = jnp.max(msg[:, 64, 0].astype(F32)) > 0.5

    def bucketed(msg, own, slot, *_):
        table = kernel_rows(jnp.arange(NX, dtype=jnp.int32))
        field, change = fields_and_changes(scale, place, msg, own, slot.reshape(SETS, beads // 128, 128), table)
        arrived = lax.all_to_all(change, "grid", split_axis=0, concat_axis=0, tiled=True)
        total = arrived.astype(F32).sum(axis=0).reshape(STEPS, beads)
        return total, field.reshape(4, ZDEV, 2 * NX)

    def general(msg, own, slot, *arguments):
        return any_spread(*arguments)

    return lax.cond(crowded, general, bucketed, msg, own, slot, cells_start, moves, accepted, bead_types)


def solution(mesh):
    return jax.shard_map(
        local,
        mesh=mesh,
        in_specs=(P("mol"), P(None, None, "mol"), P(None, "mol"), P("mol")),
        out_specs=(P(None, "mol"), P("mol", "grid", None)),
        check_vma=False,
    )
```

```python
import functools

import jax
import jax.numpy as jnp
from jax import lax
from jax.experimental import pallas as pl
from jax.experimental.pallas import tpu as pltpu
from jax.sharding import PartitionSpec as P

NX = 512
NY = 64
ZDEV = 4
STEPS = 2
SPREAD = 2
SLABS = 16
BANDS = 8
SLOTS = 128
CHUNK = 256
BLOCK = 1024
SETS = 4
ROWS = NY * ZDEV
MARK = 320.0
F32 = jnp.float32
BF16 = jnp.bfloat16
LANES = (((1,), (1,)), ((), ()))


chi_mix = 1.0
kappa_comp = 0.5


def split_up(x, dim, size):
    shape = x.shape
    blocks = x.reshape(*shape[:dim], size, shape[dim] // size, *shape[dim + 1 :])
    return jnp.moveaxis(blocks, dim, 0)


def sum_at_owner(x, axis, dim):
    blocks = split_up(x, dim, lax.axis_size(axis))
    arrived = lax.all_to_all(blocks, axis, split_axis=0, concat_axis=0, tiled=True)
    return arrived.sum(axis=0)


def laid_out(blocks, dim):
    blocks = jnp.moveaxis(blocks, 0, dim)
    shape = blocks.shape
    return blocks.reshape(*shape[:dim], shape[dim] * shape[dim + 1], *shape[dim + 2 :])


def sent_to_all(x, axis):
    copies = jnp.broadcast_to(x, (lax.axis_size(axis), *x.shape))
    return lax.all_to_all(copies, axis, split_axis=0, concat_axis=0, tiled=True)


def collect(x, axis, dim):
    return laid_out(sent_to_all(x, axis), dim)


def of_everyone(x, axis):
    return sent_to_all(x, axis).astype(jnp.float32).sum(axis=0)


def kernel_rows(col_x):
    column = jnp.arange(NX, dtype=jnp.float32)
    distance = jnp.abs(column[None, :] - col_x.astype(jnp.float32)[:, None])
    distance = jnp.minimum(distance, NX - distance)
    weights = jnp.exp(-distance * distance / (2.0 * SPREAD * SPREAD))
    first = jnp.abs(column)
    first = jnp.minimum(first, NX - first)
    total = jnp.sum(jnp.exp(-first * first / (2.0 * SPREAD * SPREAD)))
    return (weights / total).astype(jnp.bfloat16)


def split_cell(cells):
    col_x = cells % NX
    row_y = cells // NX % NY
    plane_z = cells // (NX * NY)
    return (col_x, row_y, plane_z)


def move_cells(cells, shift, planes):
    col_x, row_y, plane_z = split_cell(cells)
    col_x = (col_x + shift[0]) % NX
    row_y = (row_y + shift[1]) % NY
    plane_z = (plane_z + shift[2]) % planes
    return (plane_z * NY + row_y) * NX + col_x


def deposit(positions, bead_types, slab, start, count):
    col_x, row_y, plane_z = split_cell(positions)
    inside = (plane_z // ZDEV == slab) & (row_y >= start) & (row_y < start + count)
    row_id = jnp.where(inside, row_y * ZDEV + plane_z - slab * ZDEV, -1)
    bead_count = positions.shape[0]
    block_size = min(1024, bead_count)
    row_total = count * ZDEV
    targets = lax.broadcasted_iota(jnp.int32, (row_total, block_size), 0)

    def add_block(block_id, total):
        begin = block_id * block_size
        rows_here = lax.dynamic_slice_in_dim(row_id, begin, block_size)
        cols_here = lax.dynamic_slice_in_dim(col_x, begin, block_size)
        types_here = lax.dynamic_slice_in_dim(bead_types, begin, block_size)
        onehot = (rows_here[None, :] == targets).astype(jnp.bfloat16)
        spread_rows = kernel_rows(cols_here)
        zeros_bf = jnp.zeros_like(spread_rows)
        first = jnp.where(types_here[:, None] == 0, spread_rows, zeros_bf)
        second = jnp.where(types_here[:, None] == 1, spread_rows, zeros_bf)
        columns = jnp.concatenate([first, second], axis=1)
        return total + jnp.dot(onehot, columns, preferred_element_type=jnp.float32)

    empty = jnp.zeros((row_total, 2 * NX), jnp.float32)
    total = lax.fori_loop(0, bead_count // block_size, add_block, empty)
    return total.reshape(count, ZDEV, 2 * NX)


def make_field(density):
    phi_a = density[:, :, :NX]
    phi_b = density[:, :, NX:]
    excess = kappa_comp * (phi_a + phi_b - 1.0)
    field_a = chi_mix * phi_b + excess
    field_b = chi_mix * phi_a + excess
    return jnp.concatenate([field_a, field_b], axis=2).astype(jnp.bfloat16)


def make_reader(points, bead_types, z_first, z_span):
    col_x, row_y, plane_z = split_cell(points)
    local_z = plane_z - z_first
    kinds = jnp.broadcast_to(bead_types[None, :], points.shape)
    column_id = kinds * NX + col_x

    def read_beads(carry, piece, start):
        span_rows = piece.shape[0]
        flat_table = piece.reshape(-1)
        valid = (row_y >= 0) & (row_y < span_rows) & (local_z >= 0) & (local_z < z_span)
        flat_index = jnp.where(valid, (row_y * z_span + local_z) * (2 * NX) + column_id, 0)
        picked = jnp.take(flat_table, flat_index).astype(jnp.float32)
        return jnp.where(valid, picked, 0.0)

    return read_beads


def any_spread(cells_start, moves, accepted, bead_types):
    grid_count = lax.axis_size("grid")
    mol_count = lax.axis_size("mol")
    slab = lax.axis_index("grid")
    planes = ZDEV * grid_count
    bead_count = cells_start.shape[0]
    scale = NX * NY * planes / (bead_count * mol_count)
    band_rows = NY // mol_count
    positions = [cells_start]
    proposals = []
    for step in range(STEPS):
        proposed = move_cells(positions[step], moves[step], planes)
        proposals.append(proposed)
        positions.append(jnp.where(accepted[step] == 1, proposed, positions[step]))
    fields = []
    for step in range(STEPS):

        def step_term(start, count, current=positions[step]):
            return deposit(current, bead_types, slab, start, count)

        summed = sum_at_owner(step_term(jnp.int32(0), band_rows * lax.axis_size("mol")), "mol", 0)
        fields.append(make_field(scale * summed))
    changes = []
    for step in range(STEPS):
        points = jnp.stack([positions[step], proposals[step]])
        start_values = jnp.zeros(points.shape, jnp.float32)
        reader = make_reader(points, bead_types, slab * ZDEV, ZDEV)
        partial_values = reader(start_values, collect(fields[step], "mol", 0), jnp.int32(0))
        values = of_everyone(partial_values.astype(jnp.bfloat16), "grid").astype(jnp.float32)
        changes.append(values[1] - values[0])
    return (jnp.stack(changes), fields[STEPS - 1])


def one_hot(row, count, base=0):
    width = row.shape[1]
    tile = jnp.broadcast_to(row, (16, width)).astype(BF16)
    iota = lax.broadcasted_iota(jnp.int32, (16, width), 0).astype(F32)
    one = jnp.ones((16, width), BF16)
    zero = jnp.zeros((16, width), BF16)
    parts = [
        jnp.where(tile == (iota + float(base + first)).astype(BF16), one, zero)
        for first in range(0, count, 16)
    ]
    return jnp.concatenate(parts, axis=0) if len(parts) > 1 else parts[0]


def prefix_matrix():
    rows = lax.broadcasted_iota(jnp.int32, (CHUNK, CHUNK + 128), 0)
    cols = lax.broadcasted_iota(jnp.int32, (CHUNK, CHUNK + 128), 1)
    return jnp.where((rows <= cols) | (cols >= CHUNK), 1.0, 0.0).astype(BF16)


def stacked(rows, width):
    iota = lax.broadcasted_iota(jnp.int32, (16, width), 0)
    total = jnp.zeros((16, width), F32)
    for i, row in enumerate(rows):
        total = jnp.where(iota == i, jnp.broadcast_to(row, (16, width)), total)
    return total.astype(BF16)


def bucket_kernel(slab_ref, cells_ref, moves_ref, accepted_ref, types_ref, msg_ref, code_ref,
                  slabs, bands, highs, lows, ranked, prefix):
    beads = cells_ref.shape[1]
    chunks = beads // CHUNK
    slab = slab_ref[0]
    kind = types_ref[...] << 21

    def moved(cell, step):
        col_x = (cell + moves_ref[0, step : step + 1, :]) & (NX - 1)
        row_y = ((cell >> 9) + moves_ref[1, step : step + 1, :]) & (NY - 1)
        plane = ((cell >> 15) + moves_ref[2, step : step + 1, :]) & (ZDEV * SLABS - 1)
        return col_x | (row_y << 9) | (plane << 15)

    start = cells_ref[...]
    first = moved(start, 0)
    after = jnp.where(accepted_ref[0:1, :] == 1, first, start)
    second = moved(after, 1)
    code_ref[0:1, :] = start | kind
    code_ref[1:2, :] = after | kind
    code_ref[2:3, :] = first | kind
    code_ref[3:4, :] = second | kind
    c = code_ref[...]
    slabs[...] = ((c >> 17) & 15).astype(F32)
    band = (c >> 12) & 7
    bands[0:SETS, :] = band.astype(F32)
    bands[SETS : 2 * SETS, :] = jnp.where(((c >> 17) & 15) == slab, band, -64).astype(F32)
    highs[...] = (((c >> 7) & 3) * 64 + (c >> 21) * 32 + ((c >> 9) & 7) * 4 + ((c >> 15) & 3) + 1).astype(F32)
    lows[...] = (c & 127).astype(F32)
    counts = jnp.zeros((SETS * 16, 32), F32)
    upper = lax.broadcasted_iota(jnp.int32, (16, CHUNK), 0) >= BANDS
    own_row = (lax.broadcasted_iota(jnp.int32, (16, CHUNK), 0) & (BANDS - 1)).astype(F32).astype(BF16)
    one = jnp.ones((16, CHUNK), BF16)
    zero = jnp.zeros((16, CHUNK), BF16)

    def both(ref, base, lanes):
        low = jnp.broadcast_to(ref[base : base + 1, lanes], (16, CHUNK))
        high = jnp.broadcast_to(ref[base + 1 : base + 2, lanes], (16, CHUNK))
        return jnp.where(upper, high, low).astype(BF16)

    for k in range(chunks):
        lanes = slice(k * CHUNK, (k + 1) * CHUNK)
        of_slab = jnp.concatenate([one_hot(slabs[s : s + 1, lanes], 16) for s in range(SETS)], axis=0)
        of_band = jnp.where(both(bands, 0, lanes) == own_row, one, zero)
        block = one_hot(jnp.full((1, CHUNK), float(k * CHUNK // BLOCK), F32), 16)
        counts += lax.dot_general(of_slab, jnp.concatenate([of_band, block], axis=0), LANES, preferred_element_type=F32)
        ranked[k * 16 : k * 16 + 16, :] = jnp.where(both(bands, SETS, lanes) == own_row, one, zero)
    set_of = lax.broadcasted_iota(jnp.int32, counts.shape, 0) // 16
    column = lax.broadcasted_iota(jnp.int32, counts.shape, 1)
    used = (column >= 16) | (set_of == column // BANDS)
    crowded = jnp.max(jnp.where(used, counts, 0.0)) > float(SLOTS)
    prefix[...] = jnp.dot(ranked[...], prefix_matrix(), preferred_element_type=F32)
    carry = jnp.zeros((16, 128), F32)
    out = [jnp.zeros((16, SLOTS), F32), jnp.zeros((16, SLOTS), F32)]
    for k in range(chunks):
        lanes = slice(k * CHUNK, (k + 1) * CHUNK)
        mine = ranked[k * 16 : k * 16 + 16, :]
        ahead = mine.astype(F32) * (prefix[k * 16 : k * 16 + 16, 0:CHUNK] + jnp.concatenate([carry, carry], axis=1))
        carry = carry + prefix[k * 16 : k * 16 + 16, CHUNK : CHUNK + 128]
        for s in range(STEPS):
            rank = jnp.sum(ahead[s * BANDS : (s + 1) * BANDS, :], axis=0, keepdims=True) - 1.0
            low = jnp.broadcast_to(lows[s : s + 1, lanes], (16, CHUNK))
            high = jnp.broadcast_to(highs[s : s + 1, lanes], (16, CHUNK))
            inside = jnp.broadcast_to(bands[SETS + s : SETS + s + 1, lanes], (16, CHUNK)).astype(BF16)
            left = jnp.where(inside == own_row, jnp.where(upper, low, high).astype(BF16), zero)
            out[s] += lax.dot_general(left, one_hot(rank, SLOTS), LANES, preferred_element_type=F32)
    corner = (lax.broadcasted_iota(jnp.int32, (16, SLOTS), 0) == 0) & (
        lax.broadcasted_iota(jnp.int32, (16, SLOTS), 1) == 0
    )
    out[0] = jnp.where(corner & crowded, MARK, out[0])
    lists = jnp.concatenate(out, axis=0).astype(BF16)
    for j in range(SLABS):
        msg_ref[j] = lists


def rank_kernel(slab_ref, code_ref, own_ref, slot_ref, slabs, digits, ranked, prefix):
    beads = code_ref.shape[1]
    chunks = beads // CHUNK
    c = code_ref[...]
    slabs[...] = ((c >> 17) & 15).astype(F32)
    digits[0:SETS, :] = (((c >> 9) & 63) * 4 + ((c >> 15) & 3)).astype(F32)
    digits[SETS : 2 * SETS, :] = ((c >> 21) * 2 + ((c >> 8) & 1) + 1).astype(F32)
    digits[2 * SETS : 3 * SETS, :] = (c & 255).astype(F32)
    here = slab_ref[0].astype(F32)
    for s in range(SETS):
        for k in range(chunks):
            at = (s * chunks + k) * 16
            ranked[at : at + 16, :] = one_hot(slabs[s : s + 1, k * CHUNK : (k + 1) * CHUNK], 16)
    prefix[...] = jnp.dot(ranked[...], prefix_matrix(), preferred_element_type=F32)
    for s in range(SETS):
        for block in range(beads // BLOCK):
            carry = jnp.zeros((16, 128), F32)
            lists = jnp.zeros((16, SLOTS), F32)
            for k in range(block * BLOCK // CHUNK, (block + 1) * BLOCK // CHUNK):
                at = (s * chunks + k) * 16
                lanes = slice(k * CHUNK, (k + 1) * CHUNK)
                ahead = prefix[at : at + 16, 0:CHUNK] + jnp.concatenate([carry, carry], axis=1)
                carry = carry + prefix[at : at + 16, CHUNK : CHUNK + 128]
                rank = jnp.sum(ranked[at : at + 16, :].astype(F32) * ahead, axis=0, keepdims=True) - 1.0
                home = slabs[s : s + 1, lanes]
                slot = (home * float(SLOTS) + rank).astype(jnp.int32)
                for i in range(CHUNK // 128):
                    line = k * CHUNK // 128 + i
                    slot_ref[s, line : line + 1, :] = slot[:, i * 128 : (i + 1) * 128]
                held = jnp.where(home == here, rank, -1.0)
                left = stacked([digits[d * SETS + s : d * SETS + s + 1, lanes] for d in range(3)], CHUNK)
                lists += lax.dot_general(left, one_hot(held, SLOTS), LANES, preferred_element_type=F32)
            at = (s * (beads // BLOCK) + block) * 8
            own_ref[at : at + 8, :] = lists[0:8, :]


def field_kernel(scale, place_ref, msg_ref, own_ref, table_ref, field_ref, value_ref,
                 count_lo, count_hi, field, values):
    blocks = own_ref.shape[0] // (8 * SETS)
    half = ROWS * 2
    for step in range(STEPS):
        for band in range(BANDS):
            hist = jnp.zeros((256, SLOTS), F32)
            for j in range(0, SLABS, 2):
                at = step * 16 + band
                high = [msg_ref[i, at : at + 1, :].astype(F32) for i in (j, j + 1)]
                low = [msg_ref[i, at + BANDS : at + BANDS + 1, :].astype(F32) for i in (j, j + 1)]
                hist += lax.dot_general(
                    one_hot(jnp.concatenate(high, axis=1), 256, 1),
                    one_hot(jnp.concatenate(low, axis=1), 128),
                    LANES,
                    preferred_element_type=F32,
                )
            upper = jnp.floor(hist * (1.0 / 256.0))
            lower = hist - 256.0 * upper
            for q in range(4):
                for t in range(2):
                    at = step * half + t * ROWS + band * 32
                    rows = slice(q * 64 + t * 32, q * 64 + t * 32 + 32)
                    count_lo[at : at + 32, q * 128 : (q + 1) * 128] = lower[rows, :].astype(BF16)
                    count_hi[at : at + 32, q * 128 : (q + 1) * 128] = upper[rows, :].astype(BF16)

    def mixed(phi_a, phi_b):
        excess = kappa_comp * (phi_a + phi_b - 1.0)
        return (chi_mix * phi_b + excess).astype(BF16), (chi_mix * phi_a + excess).astype(BF16)

    table = table_ref[...]
    for step in range(STEPS):
        rows = slice(step * half, (step + 1) * half)
        dens = lax.dot_general(table, count_lo[rows, :], LANES, preferred_element_type=F32)
        dens += 256.0 * lax.dot_general(table, count_hi[rows, :], LANES, preferred_element_type=F32)
        dens = dens * scale
        field_a, field_b = mixed(dens[:, 0:ROWS], dens[:, ROWS:])
        field[step, :, 0:ROWS] = field_a
        field[step, :, ROWS:] = field_b
    at = (STEPS - 1) * half + place_ref[0] * 16
    mine = []
    for t in range(2):
        rows = pl.ds(pl.multiple_of(at + t * ROWS, 16), 16)
        dens = jnp.dot(count_lo[rows, :], table, preferred_element_type=F32)
        dens += 256.0 * jnp.dot(count_hi[rows, :], table, preferred_element_type=F32)
        mine.append(dens * scale)
    for t, part in enumerate(mixed(*mine)):
        for y in range(4):
            field_ref[y, :, t * NX : (t + 1) * NX] = part[y * ZDEV : (y + 1) * ZDEV, :]
    column = lax.broadcasted_iota(jnp.int32, (256, CHUNK), 0).astype(F32)
    for step in range(STEPS):
        for which in range(2):
            for block in range(0, blocks, 2):
                at = ((which * STEPS + step) * blocks + block) * 8

                def digit(d):
                    return jnp.concatenate([own_ref[at + d : at + d + 1, :], own_ref[at + 8 + d : at + 9 + d, :]], axis=1)

                row, part, low = digit(0), digit(1), digit(2)
                picked = jnp.zeros((256, CHUNK), F32)
                for q in range(4):
                    x_at, t_at = (q & 1) * 256, (q >> 1) * ROWS
                    picked += jnp.dot(
                        field[step, x_at : x_at + 256, t_at : t_at + ROWS],
                        one_hot(jnp.where(part == q + 1.0, row, -1.0), ROWS),
                        preferred_element_type=F32,
                    )
                got = jnp.sum(jnp.where(column == low, picked, 0.0), axis=0, keepdims=True)
                to = (step * 2 + which) * blocks + block
                values[to : to + 1, :] = got[:, 0:SLOTS]
                values[to + 1 : to + 2, :] = got[:, SLOTS:]
    lists = values[...].astype(BF16)
    for j in range(SLABS):
        value_ref[j] = lists


def change_kernel(value_ref, slot_ref, field_in_ref, change_ref, field_ref):
    lines = slot_ref.shape[1]
    blocks = lines * 128 // BLOCK
    for step in range(STEPS):
        for block in range(blocks):
            back = []
            for which in range(2):
                slot = slot_ref[which * STEPS + step, block * 8 : block * 8 + 8, :]
                rank = slot & (SLOTS - 1)
                home = slot >> 7
                at = (step * 2 + which) * blocks + block
                total = jnp.zeros((8, 128), F32)
                for j in range(SLABS):
                    line = jnp.broadcast_to(value_ref[j, at : at + 1, :].astype(F32), (8, 128))
                    total = jnp.where(home == j, jnp.take_along_axis(line, rank, axis=1), total)
                back.append(total)
            change = back[1] - back[0]
            for i in range(8):
                lanes = slice((block * 8 + i) * 128, (block * 8 + i + 1) * 128)
                change_ref[step : step + 1, lanes] = change[i : i + 1, :]
    field_ref[...] = field_in_ref[...]


VMEM = pl.BlockSpec(memory_space=pltpu.VMEM)
SMEM = pl.BlockSpec(memory_space=pltpu.SMEM)


def shape(dims, dtype):
    return jax.ShapeDtypeStruct(dims, dtype)


def local(cells_start, moves, accepted, bead_types):
    beads = cells_start.shape[0]
    chunks = beads // CHUNK
    blocks = beads // BLOCK
    slab = lax.axis_index("grid").astype(jnp.int32).reshape(1)
    place = lax.axis_index("mol").astype(jnp.int32).reshape(1)
    scale = NX * NY * ZDEV * SLABS / (beads * lax.axis_size("mol"))
    msg, code = pl.pallas_call(
        bucket_kernel,
        out_shape=(shape((SLABS, 32, SLOTS), BF16), shape((SETS, beads), jnp.int32)),
        in_specs=[SMEM] + [VMEM] * 4,
        out_specs=(VMEM, VMEM),
        scratch_shapes=[
            pltpu.VMEM((SETS, beads), F32),
            pltpu.VMEM((2 * SETS, beads), F32),
            pltpu.VMEM((SETS, beads), F32),
            pltpu.VMEM((SETS, beads), F32),
            pltpu.VMEM((chunks * 16, CHUNK), BF16),
            pltpu.VMEM((chunks * 16, CHUNK + 128), F32),
        ],
        name="bucket",
    )(slab, cells_start.reshape(1, beads), jnp.moveaxis(moves, 1, 0), accepted, bead_types.reshape(1, beads))
    msg = lax.all_to_all(msg, "mol", split_axis=0, concat_axis=0, tiled=True)
    own, slot = pl.pallas_call(
        rank_kernel,
        out_shape=(shape((SETS * blocks * 8, SLOTS), F32), shape((SETS, beads // 128, 128), jnp.int32)),
        in_specs=[SMEM, VMEM],
        out_specs=(VMEM, VMEM),
        scratch_shapes=[
            pltpu.VMEM((SETS, beads), F32),
            pltpu.VMEM((3 * SETS, beads), F32),
            pltpu.VMEM((SETS * chunks * 16, CHUNK), BF16),
            pltpu.VMEM((SETS * chunks * 16, CHUNK + 128), F32),
        ],
        name="ranks",
    )(slab, code)
    table = kernel_rows(jnp.arange(NX, dtype=jnp.int32))
    field, value = pl.pallas_call(
        functools.partial(field_kernel, scale),
        out_shape=(shape((4, ZDEV, 2 * NX), BF16), shape((SLABS, SETS * blocks, SLOTS), BF16)),
        in_specs=[SMEM] + [VMEM] * 3,
        out_specs=(VMEM, VMEM),
        scratch_shapes=[
            pltpu.VMEM((STEPS * ROWS * 2, NX), BF16),
            pltpu.VMEM((STEPS * ROWS * 2, NX), BF16),
            pltpu.VMEM((STEPS, NX, ROWS * 2), BF16),
            pltpu.VMEM((SETS * blocks, SLOTS), F32),
        ],
        name="fields",
    )(place, msg, own, table)
    value = lax.all_to_all(value, "grid", split_axis=0, concat_axis=0, tiled=True)
    crowded = jnp.max(msg[:, 0, 0].astype(F32)) >= MARK

    def bucketed(value, slot, field, *_):
        return pl.pallas_call(
            change_kernel,
            out_shape=(shape((STEPS, beads), F32), shape(field.shape, BF16)),
            in_specs=[VMEM] * 3,
            out_specs=(VMEM, VMEM),
            name="changes",
        )(value, slot, field)

    def general(value, slot, field, *arguments):
        return any_spread(*arguments)

    return lax.cond(crowded, general, bucketed, value, slot, field, cells_start, moves, accepted, bead_types)


def solution(mesh):
    return jax.shard_map(
        local,
        mesh=mesh,
        in_specs=(P("mol"), P(None, None, "mol"), P(None, "mol"), P("mol")),
        out_specs=(P(None, "mol"), P("mol", "grid", None)),
        check_vma=False,
    )
```

```python
import functools

import jax
import jax.numpy as jnp
from jax import lax
from jax.experimental import pallas as pl
from jax.experimental.pallas import tpu as pltpu
from jax.sharding import PartitionSpec as P

NX = 512
NY = 64
ZDEV = 4
STEPS = 2
SPREAD = 2
SLABS = 16
BANDS = 16
SLOTS = 128
ROOMS = 64
CHUNK = 256
BLOCK = 1024
SETS = 4
ROWS = NY * ZDEV
MARK = 320.0
F32 = jnp.float32
BF16 = jnp.bfloat16
LANES = (((1,), (1,)), ((), ()))


chi_mix = 1.0
kappa_comp = 0.5


def split_up(x, dim, size):
    shape = x.shape
    blocks = x.reshape(*shape[:dim], size, shape[dim] // size, *shape[dim + 1 :])
    return jnp.moveaxis(blocks, dim, 0)


def sum_at_owner(x, axis, dim):
    blocks = split_up(x, dim, lax.axis_size(axis))
    arrived = lax.all_to_all(blocks, axis, split_axis=0, concat_axis=0, tiled=True)
    return arrived.sum(axis=0)


def laid_out(blocks, dim):
    blocks = jnp.moveaxis(blocks, 0, dim)
    shape = blocks.shape
    return blocks.reshape(*shape[:dim], shape[dim] * shape[dim + 1], *shape[dim + 2 :])


def sent_to_all(x, axis):
    copies = jnp.broadcast_to(x, (lax.axis_size(axis), *x.shape))
    return lax.all_to_all(copies, axis, split_axis=0, concat_axis=0, tiled=True)


def collect(x, axis, dim):
    return laid_out(sent_to_all(x, axis), dim)


def of_everyone(x, axis):
    return sent_to_all(x, axis).astype(jnp.float32).sum(axis=0)


def kernel_rows(col_x):
    column = jnp.arange(NX, dtype=jnp.float32)
    distance = jnp.abs(column[None, :] - col_x.astype(jnp.float32)[:, None])
    distance = jnp.minimum(distance, NX - distance)
    weights = jnp.exp(-distance * distance / (2.0 * SPREAD * SPREAD))
    first = jnp.abs(column)
    first = jnp.minimum(first, NX - first)
    total = jnp.sum(jnp.exp(-first * first / (2.0 * SPREAD * SPREAD)))
    return (weights / total).astype(jnp.bfloat16)


def split_cell(cells):
    col_x = cells % NX
    row_y = cells // NX % NY
    plane_z = cells // (NX * NY)
    return (col_x, row_y, plane_z)


def move_cells(cells, shift, planes):
    col_x, row_y, plane_z = split_cell(cells)
    col_x = (col_x + shift[0]) % NX
    row_y = (row_y + shift[1]) % NY
    plane_z = (plane_z + shift[2]) % planes
    return (plane_z * NY + row_y) * NX + col_x


def deposit(positions, bead_types, slab, start, count):
    col_x, row_y, plane_z = split_cell(positions)
    inside = (plane_z // ZDEV == slab) & (row_y >= start) & (row_y < start + count)
    row_id = jnp.where(inside, row_y * ZDEV + plane_z - slab * ZDEV, -1)
    bead_count = positions.shape[0]
    block_size = min(1024, bead_count)
    row_total = count * ZDEV
    targets = lax.broadcasted_iota(jnp.int32, (row_total, block_size), 0)

    def add_block(block_id, total):
        begin = block_id * block_size
        rows_here = lax.dynamic_slice_in_dim(row_id, begin, block_size)
        cols_here = lax.dynamic_slice_in_dim(col_x, begin, block_size)
        types_here = lax.dynamic_slice_in_dim(bead_types, begin, block_size)
        onehot = (rows_here[None, :] == targets).astype(jnp.bfloat16)
        spread_rows = kernel_rows(cols_here)
        zeros_bf = jnp.zeros_like(spread_rows)
        first = jnp.where(types_here[:, None] == 0, spread_rows, zeros_bf)
        second = jnp.where(types_here[:, None] == 1, spread_rows, zeros_bf)
        columns = jnp.concatenate([first, second], axis=1)
        return total + jnp.dot(onehot, columns, preferred_element_type=jnp.float32)

    empty = jnp.zeros((row_total, 2 * NX), jnp.float32)
    total = lax.fori_loop(0, bead_count // block_size, add_block, empty)
    return total.reshape(count, ZDEV, 2 * NX)


def make_field(density):
    phi_a = density[:, :, :NX]
    phi_b = density[:, :, NX:]
    excess = kappa_comp * (phi_a + phi_b - 1.0)
    field_a = chi_mix * phi_b + excess
    field_b = chi_mix * phi_a + excess
    return jnp.concatenate([field_a, field_b], axis=2).astype(jnp.bfloat16)


def make_reader(points, bead_types, z_first, z_span):
    col_x, row_y, plane_z = split_cell(points)
    local_z = plane_z - z_first
    kinds = jnp.broadcast_to(bead_types[None, :], points.shape)
    column_id = kinds * NX + col_x

    def read_beads(carry, piece, start):
        span_rows = piece.shape[0]
        flat_table = piece.reshape(-1)
        valid = (row_y >= 0) & (row_y < span_rows) & (local_z >= 0) & (local_z < z_span)
        flat_index = jnp.where(valid, (row_y * z_span + local_z) * (2 * NX) + column_id, 0)
        picked = jnp.take(flat_table, flat_index).astype(jnp.float32)
        return jnp.where(valid, picked, 0.0)

    return read_beads


def any_spread(cells_start, moves, accepted, bead_types):
    grid_count = lax.axis_size("grid")
    mol_count = lax.axis_size("mol")
    slab = lax.axis_index("grid")
    planes = ZDEV * grid_count
    bead_count = cells_start.shape[0]
    scale = NX * NY * planes / (bead_count * mol_count)
    band_rows = NY // mol_count
    positions = [cells_start]
    proposals = []
    for step in range(STEPS):
        proposed = move_cells(positions[step], moves[step], planes)
        proposals.append(proposed)
        positions.append(jnp.where(accepted[step] == 1, proposed, positions[step]))
    fields = []
    for step in range(STEPS):

        def step_term(start, count, current=positions[step]):
            return deposit(current, bead_types, slab, start, count)

        summed = sum_at_owner(step_term(jnp.int32(0), band_rows * lax.axis_size("mol")), "mol", 0)
        fields.append(make_field(scale * summed))
    changes = []
    for step in range(STEPS):
        points = jnp.stack([positions[step], proposals[step]])
        start_values = jnp.zeros(points.shape, jnp.float32)
        reader = make_reader(points, bead_types, slab * ZDEV, ZDEV)
        partial_values = reader(start_values, collect(fields[step], "mol", 0), jnp.int32(0))
        values = of_everyone(partial_values.astype(jnp.bfloat16), "grid").astype(jnp.float32)
        changes.append(values[1] - values[0])
    return (jnp.stack(changes), fields[STEPS - 1])


def one_hot(row, count, base=0):
    width = row.shape[1]
    tile = jnp.broadcast_to(row, (16, width)).astype(BF16)
    iota = lax.broadcasted_iota(jnp.int32, (16, width), 0).astype(F32)
    one = jnp.ones((16, width), BF16)
    zero = jnp.zeros((16, width), BF16)
    parts = [
        jnp.where(tile == (iota + float(base + first)).astype(BF16), one, zero)
        for first in range(0, count, 16)
    ]
    return jnp.concatenate(parts, axis=0) if len(parts) > 1 else parts[0]


def prefix_matrix():
    rows = lax.broadcasted_iota(jnp.int32, (CHUNK, CHUNK + 128), 0)
    cols = lax.broadcasted_iota(jnp.int32, (CHUNK, CHUNK + 128), 1)
    return jnp.where((rows <= cols) | (cols >= CHUNK), 1.0, 0.0).astype(BF16)


def stacked(rows, width):
    iota = lax.broadcasted_iota(jnp.int32, (16, width), 0)
    total = jnp.zeros((16, width), F32)
    for i, row in enumerate(rows):
        total = jnp.where(iota == i, jnp.broadcast_to(row, (16, width)), total)
    return total.astype(BF16)


def bucket_kernel(slab_ref, cells_ref, moves_ref, accepted_ref, types_ref, msg_ref, code_ref,
                  slabs, bands, highs, lows, ranked, prefix):
    beads = cells_ref.shape[1]
    chunks = beads // CHUNK
    slab = slab_ref[0]
    kind = types_ref[...] << 21

    def moved(cell, step):
        col_x = (cell + moves_ref[0, step : step + 1, :]) & (NX - 1)
        row_y = ((cell >> 9) + moves_ref[1, step : step + 1, :]) & (NY - 1)
        plane = ((cell >> 15) + moves_ref[2, step : step + 1, :]) & (ZDEV * SLABS - 1)
        return col_x | (row_y << 9) | (plane << 15)

    start = cells_ref[...]
    first = moved(start, 0)
    after = jnp.where(accepted_ref[0:1, :] == 1, first, start)
    second = moved(after, 1)
    code_ref[0:1, :] = start | kind
    code_ref[1:2, :] = after | kind
    code_ref[2:3, :] = first | kind
    code_ref[3:4, :] = second | kind
    c = code_ref[...]
    slabs[...] = ((c >> 17) & 15).astype(F32)
    band = (c >> 11) & 15
    inside = ((c >> 17) & 15) == slab
    bands[0:SETS, :] = band.astype(F32)
    bands[SETS : 2 * SETS, :] = jnp.where(inside, band, -64).astype(F32)
    bands[2 * SETS : 3 * SETS, :] = jnp.where(inside, band & 7, -64).astype(F32)
    bands[3 * SETS : 4 * SETS, :] = ((band >> 3) * ROOMS).astype(F32)
    highs[...] = (((c >> 7) & 3) * 32 + (c >> 21) * 16 + ((c >> 9) & 3) * 4 + ((c >> 15) & 3) + 1).astype(F32)
    lows[...] = (c & 127).astype(F32)
    counts = jnp.zeros((SETS * 16, 48), F32)
    upper = lax.broadcasted_iota(jnp.int32, (16, CHUNK), 0) >= 8
    own_row = (lax.broadcasted_iota(jnp.int32, (16, CHUNK), 0) & 7).astype(F32).astype(BF16)
    zero = jnp.zeros((16, CHUNK), BF16)
    for k in range(chunks):
        lanes = slice(k * CHUNK, (k + 1) * CHUNK)
        of_slab = jnp.concatenate([one_hot(slabs[s : s + 1, lanes], 16) for s in range(SETS)], axis=0)
        kinds = [one_hot(bands[s : s + 1, lanes], 16) for s in range(STEPS)]
        kinds.append(one_hot(jnp.full((1, CHUNK), float(k * CHUNK // BLOCK), F32), 16))
        counts += lax.dot_general(of_slab, jnp.concatenate(kinds, axis=0), LANES, preferred_element_type=F32)
        for s in range(STEPS):
            at = (s * chunks + k) * 16
            ranked[at : at + 16, :] = one_hot(bands[SETS + s : SETS + s + 1, lanes], 16)
    set_of = lax.broadcasted_iota(jnp.int32, counts.shape, 0) // 16
    kind_of = lax.broadcasted_iota(jnp.int32, counts.shape, 1) // 16
    limit = jnp.where(kind_of == STEPS, float(SLOTS), jnp.where(set_of == kind_of, float(ROOMS), float(beads)))
    crowded = jnp.max(counts - limit) > 0.0
    prefix[...] = jnp.dot(ranked[...], prefix_matrix(), preferred_element_type=F32)
    out = []
    for s in range(STEPS):
        carry = jnp.zeros((16, 128), F32)
        lists = jnp.zeros((16, SLOTS), F32)
        for k in range(chunks):
            at = (s * chunks + k) * 16
            lanes = slice(k * CHUNK, (k + 1) * CHUNK)
            ahead = prefix[at : at + 16, 0:CHUNK] + jnp.concatenate([carry, carry], axis=1)
            carry = carry + prefix[at : at + 16, CHUNK : CHUNK + 128]
            rank = jnp.sum(ranked[at : at + 16, :].astype(F32) * ahead, axis=0, keepdims=True) - 1.0
            lane = jnp.where(rank >= 0.0, rank + bands[3 * SETS + s : 3 * SETS + s + 1, lanes], -1.0)
            low = jnp.broadcast_to(lows[s : s + 1, lanes], (16, CHUNK))
            high = jnp.broadcast_to(highs[s : s + 1, lanes], (16, CHUNK))
            row = jnp.broadcast_to(bands[2 * SETS + s : 2 * SETS + s + 1, lanes], (16, CHUNK)).astype(BF16)
            left = jnp.where(row == own_row, jnp.where(upper, low, high).astype(BF16), zero)
            lists += lax.dot_general(left, one_hot(lane, SLOTS), LANES, preferred_element_type=F32)
        out.append(lists)
    corner = (lax.broadcasted_iota(jnp.int32, (16, SLOTS), 0) == 0) & (
        lax.broadcasted_iota(jnp.int32, (16, SLOTS), 1) == 0
    )
    out[0] = jnp.where(corner & crowded, MARK, out[0])
    message = jnp.concatenate(out, axis=0).astype(BF16)
    for j in range(SLABS):
        msg_ref[j] = message


def rank_kernel(scale, slab_ref, code_ref, own_ref, slot_ref, table_ref, slabs, digits, ranked, prefix):
    column = lax.broadcasted_iota(jnp.int32, (8, NX), 1)
    distance = jnp.minimum(column, NX - column).astype(F32)
    weights = jnp.exp(-distance * distance / (2.0 * SPREAD * SPREAD))
    first = (weights / jnp.sum(weights[0:1, :], axis=1, keepdims=True))[0:1, :]
    turned = pltpu.roll(jnp.broadcast_to(first, (NX, NX)), 0, 1, stride=1, stride_axis=0)
    table_ref[...] = turned.astype(BF16) * jnp.full((NX, NX), scale, BF16)
    beads = code_ref.shape[1]
    chunks = beads // CHUNK
    c = code_ref[...]
    slabs[...] = ((c >> 17) & 15).astype(F32)
    digits[0:SETS, :] = (((c >> 9) & 63) * 4 + ((c >> 15) & 3)).astype(F32)
    digits[SETS : 2 * SETS, :] = ((c >> 21) * 2 + ((c >> 8) & 1) + 1).astype(F32)
    digits[2 * SETS : 3 * SETS, :] = (c & 255).astype(F32)
    here = slab_ref[0].astype(F32)
    for s in range(SETS):
        for k in range(chunks):
            at = (s * chunks + k) * 16
            ranked[at : at + 16, :] = one_hot(slabs[s : s + 1, k * CHUNK : (k + 1) * CHUNK], 16)
    prefix[...] = jnp.dot(ranked[...], prefix_matrix(), preferred_element_type=F32)
    for s in range(SETS):
        for block in range(beads // BLOCK):
            carry = jnp.zeros((16, 128), F32)
            lists = jnp.zeros((16, SLOTS), F32)
            for k in range(block * BLOCK // CHUNK, (block + 1) * BLOCK // CHUNK):
                at = (s * chunks + k) * 16
                lanes = slice(k * CHUNK, (k + 1) * CHUNK)
                ahead = prefix[at : at + 16, 0:CHUNK] + jnp.concatenate([carry, carry], axis=1)
                carry = carry + prefix[at : at + 16, CHUNK : CHUNK + 128]
                rank = jnp.sum(ranked[at : at + 16, :].astype(F32) * ahead, axis=0, keepdims=True) - 1.0
                home = slabs[s : s + 1, lanes]
                slot = (home * float(SLOTS) + rank).astype(jnp.int32)
                for i in range(CHUNK // 128):
                    line = k * CHUNK // 128 + i
                    slot_ref[s, line : line + 1, :] = slot[:, i * 128 : (i + 1) * 128]
                held = jnp.where(home == here, rank, -1.0)
                left = stacked([digits[d * SETS + s : d * SETS + s + 1, lanes] for d in range(3)], CHUNK)
                lists += lax.dot_general(left, one_hot(held, SLOTS), LANES, preferred_element_type=F32)
            at = (s * (beads // BLOCK) + block) * 8
            own_ref[at : at + 8, :] = lists[0:8, :]


def field_kernel(place_ref, msg_ref, own_ref, table_ref, field_ref, value_ref, crowd_ref,
                 slots, count, count_lo, count_hi, dens, field, values):
    blocks = own_ref.shape[0] // (8 * SETS)
    half = ROWS * 2
    marks = msg_ref[0, 0:1, :].astype(F32)
    for j in range(1, SLABS):
        marks = jnp.maximum(marks, msg_ref[j, 0:1, :].astype(F32))
    crowd_ref[0] = (jnp.max(marks) >= MARK).astype(jnp.int32)
    most = jnp.zeros((8, SLOTS), F32)
    left_half = lax.broadcasted_iota(jnp.int32, (32, SLOTS), 1) < ROOMS
    for j in range(0, SLABS, 2):
        even, odd = msg_ref[j].astype(F32), msg_ref[j + 1].astype(F32)
        lanes = slice(j // 2 * SLOTS, (j // 2 + 1) * SLOTS)
        slots[0, :, lanes] = jnp.where(left_half, even, pltpu.roll(odd, ROOMS, 1))
        slots[1, :, lanes] = jnp.where(left_half, pltpu.roll(even, ROOMS, 1), odd)
    for step in range(STEPS):
        for band in range(BANDS):
            hist = jnp.zeros((128, 128), F32)
            at = step * 16 + band % 8
            for k in range(0, slots.shape[2], CHUNK):
                hist += lax.dot_general(
                    one_hot(slots[band // 8, at : at + 1, k : k + CHUNK], 128, 1),
                    one_hot(slots[band // 8, at + 8 : at + 9, k : k + CHUNK], 128),
                    LANES,
                    preferred_element_type=F32,
                )
            for q in range(4):
                for t in range(2):
                    at = step * half + t * ROWS + band * 16
                    part = hist[q * 32 + t * 16 : q * 32 + t * 16 + 16, :]
                    count[at : at + 16, q * 128 : (q + 1) * 128] = part
                    count_lo[at : at + 16, q * 128 : (q + 1) * 128] = part.astype(BF16)
                    most = jnp.maximum(most, jnp.maximum(part[0:8, :], part[8:16, :]))
    many = jnp.max(most) > 256.0

    def mixed(phi_a, phi_b):
        excess = kappa_comp * (phi_a + phi_b - 1.0)
        return (chi_mix * phi_b + excess).astype(BF16), (chi_mix * phi_a + excess).astype(BF16)

    def whole(counts):
        return [
            lax.dot_general(table_ref[...], counts[step * half : (step + 1) * half, :], LANES, preferred_element_type=F32)
            for step in range(STEPS)
        ]

    def own(digit):
        at = (STEPS - 1) * half + place_ref[0] * 16
        return [
            jnp.dot(
                digit(count[pl.ds(pl.multiple_of(at + t * ROWS, 16), 16), :]).astype(BF16),
                table_ref[...],
                preferred_element_type=F32,
            )
            for t in range(2)
        ]

    def store_fields(dens, mine):
        for step in range(STEPS):
            field_a, field_b = mixed(dens[step][:, 0:ROWS], dens[step][:, ROWS:])
            field[step, :, 0:ROWS] = field_a
            field[step, :, ROWS:] = field_b
        for t, part in enumerate(mixed(*mine)):
            for y in range(4):
                field_ref[y, :, t * NX : (t + 1) * NX] = part[y * ZDEV : (y + 1) * ZDEV, :]

    def upper(rows):
        return jnp.floor(rows * (1.0 / 256.0))

    def lower(rows):
        return rows - 256.0 * upper(rows)

    @pl.when(jnp.logical_not(many))
    def _():
        store_fields(whole(count_lo), own(lambda rows: rows))

    @pl.when(many)
    def _():
        for i in range(0, STEPS * half, 64):
            count_lo[i : i + 64, :] = lower(count[i : i + 64, :]).astype(BF16)
            count_hi[i : i + 64, :] = upper(count[i : i + 64, :]).astype(BF16)
        for step, part in enumerate(whole(count_hi)):
            dens[step] = 256.0 * part
        store_fields(
            [dens[step] + part for step, part in enumerate(whole(count_lo))],
            [256.0 * a + b for a, b in zip(own(upper), own(lower))],
        )

    column = lax.broadcasted_iota(jnp.int32, (256, CHUNK), 0).astype(F32)
    for step in range(STEPS):
        for which in range(2):
            for block in range(0, blocks, 2):
                at = ((which * STEPS + step) * blocks + block) * 8

                def digit(d):
                    return jnp.concatenate([own_ref[at + d : at + d + 1, :], own_ref[at + 8 + d : at + 9 + d, :]], axis=1)

                row, part, low = digit(0), digit(1), digit(2)
                picked = jnp.zeros((256, CHUNK), F32)
                for q in range(4):
                    x_at, t_at = (q & 1) * 256, (q >> 1) * ROWS
                    picked += jnp.dot(
                        field[step, x_at : x_at + 256, t_at : t_at + ROWS],
                        one_hot(jnp.where(part == q + 1.0, row, -1.0), ROWS),
                        preferred_element_type=F32,
                    )
                got = jnp.sum(jnp.where(column == low, picked, 0.0), axis=0, keepdims=True)
                to = (step * 2 + which) * blocks + block
                values[to : to + 1, :] = got[:, 0:SLOTS]
                values[to + 1 : to + 2, :] = got[:, SLOTS:]
    lists = values[...].astype(BF16)
    for j in range(SLABS):
        value_ref[j] = lists


def change_kernel(value_ref, slot_ref, field_in_ref, change_out, field_out, change_ref, sems):
    field_copy = pltpu.make_async_copy(field_in_ref, field_out, sems.at[0])
    field_copy.start()
    lines = slot_ref.shape[1]
    blocks = lines * 128 // BLOCK
    for step in range(STEPS):
        for block in range(blocks):
            back = []
            for which in range(2):
                slot = slot_ref[which * STEPS + step, block * 8 : block * 8 + 8, :]
                rank = slot & (SLOTS - 1)
                home = slot >> 7
                at = (step * 2 + which) * blocks + block
                total = jnp.zeros((8, 128), F32)
                for j in range(SLABS):
                    line = jnp.broadcast_to(value_ref[j, at : at + 1, :].astype(F32), (8, 128))
                    total = jnp.where(home == j, jnp.take_along_axis(line, rank, axis=1), total)
                back.append(total)
            change = back[1] - back[0]
            for i in range(8):
                lanes = slice((block * 8 + i) * 128, (block * 8 + i + 1) * 128)
                change_ref[step : step + 1, lanes] = change[i : i + 1, :]
    change_copy = pltpu.make_async_copy(change_ref, change_out, sems.at[1])
    change_copy.start()
    field_copy.wait()
    change_copy.wait()


VMEM = pl.BlockSpec(memory_space=pltpu.VMEM)
SMEM = pl.BlockSpec(memory_space=pltpu.SMEM)
HBM = pl.BlockSpec(memory_space=pltpu.HBM)
ROOM = pltpu.CompilerParams(vmem_limit_bytes=24 * 2**20)


def shape(dims, dtype):
    return jax.ShapeDtypeStruct(dims, dtype)


def local(cells_start, moves, accepted, bead_types):
    beads = cells_start.shape[0]
    chunks = beads // CHUNK
    blocks = beads // BLOCK
    slab = lax.axis_index("grid").astype(jnp.int32).reshape(1)
    place = lax.axis_index("mol").astype(jnp.int32).reshape(1)
    scale = NX * NY * ZDEV * SLABS / (beads * lax.axis_size("mol"))
    msg, code = pl.pallas_call(
        bucket_kernel,
        out_shape=(shape((SLABS, 32, SLOTS), BF16), shape((SETS, beads), jnp.int32)),
        in_specs=[SMEM] + [VMEM] * 4,
        out_specs=(VMEM, VMEM),
        compiler_params=ROOM,
        scratch_shapes=[
            pltpu.VMEM((SETS, beads), F32),
            pltpu.VMEM((4 * SETS, beads), F32),
            pltpu.VMEM((SETS, beads), F32),
            pltpu.VMEM((SETS, beads), F32),
            pltpu.VMEM((STEPS * chunks * 16, CHUNK), BF16),
            pltpu.VMEM((STEPS * chunks * 16, CHUNK + 128), F32),
        ],
        name="bucket",
    )(slab, cells_start.reshape(1, beads), jnp.moveaxis(moves, 1, 0), accepted, bead_types.reshape(1, beads))
    msg = lax.all_to_all(msg, "mol", split_axis=0, concat_axis=0, tiled=True)
    own, slot, table = pl.pallas_call(
        functools.partial(rank_kernel, scale),
        out_shape=(
            shape((SETS * blocks * 8, SLOTS), F32),
            shape((SETS, beads // 128, 128), jnp.int32),
            shape((NX, NX), BF16),
        ),
        in_specs=[SMEM, VMEM],
        out_specs=(VMEM, VMEM, VMEM),
        compiler_params=ROOM,
        scratch_shapes=[
            pltpu.VMEM((SETS, beads), F32),
            pltpu.VMEM((3 * SETS, beads), F32),
            pltpu.VMEM((SETS * chunks * 16, CHUNK), BF16),
            pltpu.VMEM((SETS * chunks * 16, CHUNK + 128), F32),
        ],
        name="ranks",
    )(slab, code)
    field, value, crowd = pl.pallas_call(
        field_kernel,
        out_shape=(
            shape((4, ZDEV, 2 * NX), BF16),
            shape((SLABS, SETS * blocks, SLOTS), BF16),
            shape((1,), jnp.int32),
        ),
        in_specs=[SMEM] + [VMEM] * 3,
        out_specs=(VMEM, VMEM, SMEM),
        compiler_params=ROOM,
        scratch_shapes=[
            pltpu.VMEM((2, 32, SLABS * ROOMS), F32),
            pltpu.VMEM((STEPS * ROWS * 2, NX), F32),
            pltpu.VMEM((STEPS * ROWS * 2, NX), BF16),
            pltpu.VMEM((STEPS * ROWS * 2, NX), BF16),
            pltpu.VMEM((STEPS, NX, ROWS * 2), F32),
            pltpu.VMEM((STEPS, NX, ROWS * 2), BF16),
            pltpu.VMEM((SETS * blocks, SLOTS), F32),
        ],
        name="fields",
    )(place, msg, own, table)
    value = lax.all_to_all(value, "grid", split_axis=0, concat_axis=0, tiled=True)

    def bucketed(value, slot, field, *_):
        return pl.pallas_call(
            change_kernel,
            out_shape=(shape((STEPS, beads), F32), shape(field.shape, BF16)),
            in_specs=[VMEM] * 3,
            out_specs=(HBM, HBM),
            scratch_shapes=[pltpu.VMEM((STEPS, beads), F32), pltpu.SemaphoreType.DMA((2,))],
            compiler_params=ROOM,
            name="changes",
        )(value, slot, field)

    def general(value, slot, field, *arguments):
        return any_spread(*arguments)

    return lax.cond(crowd[0] == 1, general, bucketed, value, slot, field, cells_start, moves, accepted, bead_types)


def solution(mesh):
    return jax.shard_map(
        local,
        mesh=mesh,
        in_specs=(P("mol"), P(None, None, "mol"), P(None, "mol"), P("mol")),
        out_specs=(P(None, "mol"), P("mol", "grid", None)),
        check_vma=False,
    )
```

```python
import functools

import jax
import jax.numpy as jnp
from jax import lax
from jax.experimental import pallas as pl
from jax.experimental.pallas import tpu as pltpu
from jax.sharding import PartitionSpec as P

NX = 512
NY = 64
ZDEV = 4
STEPS = 2
SPREAD = 2
SLABS = 16
BANDS = 16
SLOTS = 128
ROOMS = 64
CHUNK = 256
BLOCK = 1024
SETS = 4
ROWS = NY * ZDEV
MARK = 320.0
F32 = jnp.float32
BF16 = jnp.bfloat16
LANES = (((1,), (1,)), ((), ()))


chi_mix = 1.0
kappa_comp = 0.5


def split_up(x, dim, size):
    shape = x.shape
    blocks = x.reshape(*shape[:dim], size, shape[dim] // size, *shape[dim + 1 :])
    return jnp.moveaxis(blocks, dim, 0)


def sum_at_owner(x, axis, dim):
    blocks = split_up(x, dim, lax.axis_size(axis))
    arrived = lax.all_to_all(blocks, axis, split_axis=0, concat_axis=0, tiled=True)
    return arrived.sum(axis=0)


def laid_out(blocks, dim):
    blocks = jnp.moveaxis(blocks, 0, dim)
    shape = blocks.shape
    return blocks.reshape(*shape[:dim], shape[dim] * shape[dim + 1], *shape[dim + 2 :])


def sent_to_all(x, axis):
    copies = jnp.broadcast_to(x, (lax.axis_size(axis), *x.shape))
    return lax.all_to_all(copies, axis, split_axis=0, concat_axis=0, tiled=True)


def collect(x, axis, dim):
    return laid_out(sent_to_all(x, axis), dim)


def of_everyone(x, axis):
    return sent_to_all(x, axis).astype(jnp.float32).sum(axis=0)


def kernel_rows(col_x):
    column = jnp.arange(NX, dtype=jnp.float32)
    distance = jnp.abs(column[None, :] - col_x.astype(jnp.float32)[:, None])
    distance = jnp.minimum(distance, NX - distance)
    weights = jnp.exp(-distance * distance / (2.0 * SPREAD * SPREAD))
    first = jnp.abs(column)
    first = jnp.minimum(first, NX - first)
    total = jnp.sum(jnp.exp(-first * first / (2.0 * SPREAD * SPREAD)))
    return (weights / total).astype(jnp.bfloat16)


def split_cell(cells):
    col_x = cells % NX
    row_y = cells // NX % NY
    plane_z = cells // (NX * NY)
    return (col_x, row_y, plane_z)


def move_cells(cells, shift, planes):
    col_x, row_y, plane_z = split_cell(cells)
    col_x = (col_x + shift[0]) % NX
    row_y = (row_y + shift[1]) % NY
    plane_z = (plane_z + shift[2]) % planes
    return (plane_z * NY + row_y) * NX + col_x


def deposit(positions, bead_types, slab, start, count):
    col_x, row_y, plane_z = split_cell(positions)
    inside = (plane_z // ZDEV == slab) & (row_y >= start) & (row_y < start + count)
    row_id = jnp.where(inside, row_y * ZDEV + plane_z - slab * ZDEV, -1)
    bead_count = positions.shape[0]
    block_size = min(1024, bead_count)
    row_total = count * ZDEV
    targets = lax.broadcasted_iota(jnp.int32, (row_total, block_size), 0)

    def add_block(block_id, total):
        begin = block_id * block_size
        rows_here = lax.dynamic_slice_in_dim(row_id, begin, block_size)
        cols_here = lax.dynamic_slice_in_dim(col_x, begin, block_size)
        types_here = lax.dynamic_slice_in_dim(bead_types, begin, block_size)
        onehot = (rows_here[None, :] == targets).astype(jnp.bfloat16)
        spread_rows = kernel_rows(cols_here)
        zeros_bf = jnp.zeros_like(spread_rows)
        first = jnp.where(types_here[:, None] == 0, spread_rows, zeros_bf)
        second = jnp.where(types_here[:, None] == 1, spread_rows, zeros_bf)
        columns = jnp.concatenate([first, second], axis=1)
        return total + jnp.dot(onehot, columns, preferred_element_type=jnp.float32)

    empty = jnp.zeros((row_total, 2 * NX), jnp.float32)
    total = lax.fori_loop(0, bead_count // block_size, add_block, empty)
    return total.reshape(count, ZDEV, 2 * NX)


def make_field(density):
    phi_a = density[:, :, :NX]
    phi_b = density[:, :, NX:]
    excess = kappa_comp * (phi_a + phi_b - 1.0)
    field_a = chi_mix * phi_b + excess
    field_b = chi_mix * phi_a + excess
    return jnp.concatenate([field_a, field_b], axis=2).astype(jnp.bfloat16)


def make_reader(points, bead_types, z_first, z_span):
    col_x, row_y, plane_z = split_cell(points)
    local_z = plane_z - z_first
    kinds = jnp.broadcast_to(bead_types[None, :], points.shape)
    column_id = kinds * NX + col_x

    def read_beads(carry, piece, start):
        span_rows = piece.shape[0]
        flat_table = piece.reshape(-1)
        valid = (row_y >= 0) & (row_y < span_rows) & (local_z >= 0) & (local_z < z_span)
        flat_index = jnp.where(valid, (row_y * z_span + local_z) * (2 * NX) + column_id, 0)
        picked = jnp.take(flat_table, flat_index).astype(jnp.float32)
        return jnp.where(valid, picked, 0.0)

    return read_beads


def any_spread(cells_start, moves, accepted, bead_types):
    grid_count = lax.axis_size("grid")
    mol_count = lax.axis_size("mol")
    slab = lax.axis_index("grid")
    planes = ZDEV * grid_count
    bead_count = cells_start.shape[0]
    scale = NX * NY * planes / (bead_count * mol_count)
    band_rows = NY // mol_count
    positions = [cells_start]
    proposals = []
    for step in range(STEPS):
        proposed = move_cells(positions[step], moves[step], planes)
        proposals.append(proposed)
        positions.append(jnp.where(accepted[step] == 1, proposed, positions[step]))
    fields = []
    for step in range(STEPS):

        def step_term(start, count, current=positions[step]):
            return deposit(current, bead_types, slab, start, count)

        summed = sum_at_owner(step_term(jnp.int32(0), band_rows * lax.axis_size("mol")), "mol", 0)
        fields.append(make_field(scale * summed))
    changes = []
    for step in range(STEPS):
        points = jnp.stack([positions[step], proposals[step]])
        start_values = jnp.zeros(points.shape, jnp.float32)
        reader = make_reader(points, bead_types, slab * ZDEV, ZDEV)
        partial_values = reader(start_values, collect(fields[step], "mol", 0), jnp.int32(0))
        values = of_everyone(partial_values.astype(jnp.bfloat16), "grid").astype(jnp.float32)
        changes.append(values[1] - values[0])
    return (jnp.stack(changes), fields[STEPS - 1])


def one_hot(row, count, base=0):
    width = row.shape[1]
    tile = jnp.broadcast_to(row, (16, width)).astype(BF16)
    iota = lax.broadcasted_iota(jnp.int32, (16, width), 0).astype(F32)
    one = jnp.ones((16, width), BF16)
    zero = jnp.zeros((16, width), BF16)
    parts = [
        jnp.where(tile == (iota + float(base + first)).astype(BF16), one, zero)
        for first in range(0, count, 16)
    ]
    return jnp.concatenate(parts, axis=0) if len(parts) > 1 else parts[0]


def prefix_matrix():
    rows = lax.broadcasted_iota(jnp.int32, (CHUNK, CHUNK + 128), 0)
    cols = lax.broadcasted_iota(jnp.int32, (CHUNK, CHUNK + 128), 1)
    return jnp.where((rows <= cols) | (cols >= CHUNK), 1.0, 0.0).astype(BF16)


def bucket_kernel(slab_ref, cells_ref, moves_ref, accepted_ref, types_ref, msg_ref, code_ref,
                  slabs, bands, highs, lows, ranked, prefix):
    beads = cells_ref.shape[1]
    chunks = beads // CHUNK
    slab = slab_ref[0]
    kind = types_ref[...] << 21

    def moved(cell, step):
        col_x = (cell + moves_ref[0, step : step + 1, :]) & (NX - 1)
        row_y = ((cell >> 9) + moves_ref[1, step : step + 1, :]) & (NY - 1)
        plane = ((cell >> 15) + moves_ref[2, step : step + 1, :]) & (ZDEV * SLABS - 1)
        return col_x | (row_y << 9) | (plane << 15)

    start = cells_ref[...]
    first = moved(start, 0)
    after = jnp.where(accepted_ref[0:1, :] == 1, first, start)
    second = moved(after, 1)
    code_ref[0:1, :] = start | kind
    code_ref[1:2, :] = after | kind
    code_ref[2:3, :] = first | kind
    code_ref[3:4, :] = second | kind
    c = code_ref[...]
    slabs[...] = ((c >> 17) & 15).astype(F32)
    band = (c >> 11) & 15
    inside = ((c >> 17) & 15) == slab
    bands[0:SETS, :] = band.astype(F32)
    bands[SETS : 2 * SETS, :] = jnp.where(inside, band, -64).astype(F32)
    bands[2 * SETS : 3 * SETS, :] = jnp.where(inside, band & 7, -64).astype(F32)
    bands[3 * SETS : 4 * SETS, :] = ((band >> 3) * ROOMS).astype(F32)
    highs[...] = (((c >> 7) & 3) * 32 + (c >> 21) * 16 + ((c >> 9) & 3) * 4 + ((c >> 15) & 3) + 1).astype(F32)
    lows[...] = (c & 127).astype(F32)
    counts = jnp.zeros((SETS * 16, 48), F32)
    upper = lax.broadcasted_iota(jnp.int32, (16, CHUNK), 0) >= 8
    own_row = (lax.broadcasted_iota(jnp.int32, (16, CHUNK), 0) & 7).astype(F32).astype(BF16)
    zero = jnp.zeros((16, CHUNK), BF16)
    for k in range(chunks):
        lanes = slice(k * CHUNK, (k + 1) * CHUNK)
        alone = [one_hot(slabs[s : s + 1, lanes], 16) for s in range(SETS)]
        either = [jnp.maximum(alone[s], alone[STEPS + s]) for s in range(STEPS)]
        of_slab = jnp.concatenate(alone[0:STEPS] + either, axis=0)
        kinds = [one_hot(bands[s : s + 1, lanes], 16) for s in range(STEPS)]
        kinds.append(one_hot(jnp.full((1, CHUNK), float(k * CHUNK // BLOCK), F32), 16))
        counts += lax.dot_general(of_slab, jnp.concatenate(kinds, axis=0), LANES, preferred_element_type=F32)
        for s in range(STEPS):
            at = (s * chunks + k) * 16
            ranked[at : at + 16, :] = one_hot(bands[SETS + s : SETS + s + 1, lanes], 16)
    set_of = lax.broadcasted_iota(jnp.int32, counts.shape, 0) // 16
    kind_of = lax.broadcasted_iota(jnp.int32, counts.shape, 1) // 16
    listed = (kind_of == STEPS) & (set_of >= STEPS)
    limit = jnp.where(listed, float(SLOTS), jnp.where(set_of == kind_of, float(ROOMS), float(beads)))
    crowded = jnp.max(counts - limit) > 0.0
    prefix[...] = jnp.dot(ranked[...], prefix_matrix(), preferred_element_type=F32)
    out = []
    for s in range(STEPS):
        carry = jnp.zeros((16, 128), F32)
        lists = jnp.zeros((16, SLOTS), F32)
        for k in range(chunks):
            at = (s * chunks + k) * 16
            lanes = slice(k * CHUNK, (k + 1) * CHUNK)
            ahead = prefix[at : at + 16, 0:CHUNK] + jnp.concatenate([carry, carry], axis=1)
            carry = carry + prefix[at : at + 16, CHUNK : CHUNK + 128]
            rank = jnp.sum(ranked[at : at + 16, :].astype(F32) * ahead, axis=0, keepdims=True) - 1.0
            lane = jnp.where(rank >= 0.0, rank + bands[3 * SETS + s : 3 * SETS + s + 1, lanes], -1.0)
            low = jnp.broadcast_to(lows[s : s + 1, lanes], (16, CHUNK))
            high = jnp.broadcast_to(highs[s : s + 1, lanes], (16, CHUNK))
            row = jnp.broadcast_to(bands[2 * SETS + s : 2 * SETS + s + 1, lanes], (16, CHUNK)).astype(BF16)
            left = jnp.where(row == own_row, jnp.where(upper, low, high).astype(BF16), zero)
            lists += lax.dot_general(left, one_hot(lane, SLOTS), LANES, preferred_element_type=F32)
        out.append(lists)
    corner = (lax.broadcasted_iota(jnp.int32, (16, SLOTS), 0) == 0) & (
        lax.broadcasted_iota(jnp.int32, (16, SLOTS), 1) == 0
    )
    out[0] = jnp.where(corner & crowded, MARK, out[0])
    message = jnp.concatenate(out, axis=0).astype(BF16)
    for j in range(SLABS):
        msg_ref[j] = message


def rank_kernel(scale, slab_ref, code_ref, own_ref, slot_ref, table_ref, slabs, digits, ranked, prefix):
    column = lax.broadcasted_iota(jnp.int32, (8, NX), 1)
    distance = jnp.minimum(column, NX - column).astype(F32)
    weights = jnp.exp(-distance * distance / (2.0 * SPREAD * SPREAD))
    first = (weights / jnp.sum(weights[0:1, :], axis=1, keepdims=True))[0:1, :]
    turned = pltpu.roll(jnp.broadcast_to(first, (NX, NX)), 0, 1, stride=1, stride_axis=0)
    table_ref[...] = turned.astype(BF16) * jnp.full((NX, NX), scale, BF16)
    beads = code_ref.shape[1]
    chunks = beads // CHUNK
    c = code_ref[...]
    home = (c >> 17) & 15
    slabs[...] = home.astype(F32)
    digits[0:SETS, :] = (((c >> 9) & 63) * 4 + ((c >> 15) & 3)).astype(F32)
    digits[SETS : 2 * SETS, :] = jnp.where(home == slab_ref[0], (c >> 21) * 2 + ((c >> 8) & 1) + 1, 0).astype(F32)
    digits[2 * SETS : 3 * SETS, :] = (c & 255).astype(F32)
    here = slab_ref[0].astype(F32)
    for s in range(STEPS):
        for k in range(chunks):
            at = (s * chunks + k) * 16
            lanes = slice(k * CHUNK, (k + 1) * CHUNK)
            ranked[at : at + 16, :] = jnp.maximum(
                one_hot(slabs[s : s + 1, lanes], 16), one_hot(slabs[STEPS + s : STEPS + s + 1, lanes], 16)
            )
    prefix[...] = jnp.dot(ranked[...], prefix_matrix(), preferred_element_type=F32)
    sixteen = lax.broadcasted_iota(jnp.int32, (16, CHUNK), 0).astype(F32)
    eight = lax.broadcasted_iota(jnp.int32, (8, CHUNK), 0)
    for s in range(STEPS):
        for block in range(beads // BLOCK):
            carry = jnp.zeros((16, 128), F32)
            lists = jnp.zeros((8, SLOTS), F32)
            for k in range(block * BLOCK // CHUNK, (block + 1) * BLOCK // CHUNK):
                at = (s * chunks + k) * 16
                lanes = slice(k * CHUNK, (k + 1) * CHUNK)
                ahead = prefix[at : at + 16, 0:CHUNK] + jnp.concatenate([carry, carry], axis=1)
                carry = carry + prefix[at : at + 16, CHUNK : CHUNK + 128]
                homes, ranks = [], []
                for p in (s, STEPS + s):
                    homes.append(slabs[p : p + 1, lanes])
                    mine = jnp.where(sixteen == jnp.broadcast_to(homes[-1], (16, CHUNK)), ahead, 0.0)
                    ranks.append(jnp.sum(mine, axis=0, keepdims=True) - 1.0)
                first = homes[0] * float(SLOTS) + ranks[0]
                second = jnp.where(homes[0] == homes[1], float(-SLOTS), homes[1] * float(SLOTS) + ranks[1])
                for p, slot in ((s, first.astype(jnp.int32)), (STEPS + s, second.astype(jnp.int32))):
                    for i in range(CHUNK // 128):
                        line = k * CHUNK // 128 + i
                        slot_ref[p, line : line + 1, :] = slot[:, i * 128 : (i + 1) * 128]
                held = jnp.where(homes[0] == here, ranks[0], jnp.where(homes[1] == here, ranks[1], -1.0))
                left = jnp.zeros((8, CHUNK), F32)
                for d in range(6):
                    row = d % 3 * SETS + d // 3 * STEPS + s
                    left = jnp.where(eight == d, jnp.broadcast_to(digits[row : row + 1, lanes], (8, CHUNK)), left)
                lists += lax.dot_general(left.astype(BF16), one_hot(held, SLOTS), LANES, preferred_element_type=F32)
            at = (s * (beads // BLOCK) + block) * 8
            own_ref[at : at + 8, :] = lists
    own_ref[STEPS * chunks * CHUNK // 128 :, :] = jnp.zeros((8, SLOTS), F32)


def field_kernel(place_ref, msg_ref, own_ref, table_ref, field_ref, value_ref, crowd_ref,
                 slots, count, count_lo, count_hi, dens, field, values):
    blocks = (own_ref.shape[0] - 8) // (8 * STEPS)
    half = ROWS * 2
    marks = msg_ref[0, 0:1, :].astype(F32)
    for j in range(1, SLABS):
        marks = jnp.maximum(marks, msg_ref[j, 0:1, :].astype(F32))
    crowd_ref[0] = (jnp.max(marks) >= MARK).astype(jnp.int32)
    most = jnp.zeros((8, SLOTS), F32)
    left_half = lax.broadcasted_iota(jnp.int32, (32, SLOTS), 1) < ROOMS
    for j in range(0, SLABS, 2):
        even, odd = msg_ref[j].astype(F32), msg_ref[j + 1].astype(F32)
        lanes = slice(j // 2 * SLOTS, (j // 2 + 1) * SLOTS)
        slots[0, :, lanes] = jnp.where(left_half, even, pltpu.roll(odd, ROOMS, 1))
        slots[1, :, lanes] = jnp.where(left_half, pltpu.roll(even, ROOMS, 1), odd)
    for step in range(STEPS):
        for band in range(BANDS):
            hist = jnp.zeros((128, 128), F32)
            at = step * 16 + band % 8
            for k in range(0, slots.shape[2], CHUNK):
                hist += lax.dot_general(
                    one_hot(slots[band // 8, at : at + 1, k : k + CHUNK], 128, 1),
                    one_hot(slots[band // 8, at + 8 : at + 9, k : k + CHUNK], 128),
                    LANES,
                    preferred_element_type=F32,
                )
            for q in range(4):
                for t in range(2):
                    at = step * half + t * ROWS + band * 16
                    part = hist[q * 32 + t * 16 : q * 32 + t * 16 + 16, :]
                    count[at : at + 16, q * 128 : (q + 1) * 128] = part
                    count_lo[at : at + 16, q * 128 : (q + 1) * 128] = part.astype(BF16)
                    most = jnp.maximum(most, jnp.maximum(part[0:8, :], part[8:16, :]))
    many = jnp.max(most) > 256.0

    def mixed(phi_a, phi_b):
        excess = kappa_comp * (phi_a + phi_b - 1.0)
        return (chi_mix * phi_b + excess).astype(BF16), (chi_mix * phi_a + excess).astype(BF16)

    def whole(counts):
        return [
            lax.dot_general(table_ref[...], counts[step * half : (step + 1) * half, :], LANES, preferred_element_type=F32)
            for step in range(STEPS)
        ]

    def own(digit):
        at = (STEPS - 1) * half + place_ref[0] * 16
        return [
            jnp.dot(
                digit(count[pl.ds(pl.multiple_of(at + t * ROWS, 16), 16), :]).astype(BF16),
                table_ref[...],
                preferred_element_type=F32,
            )
            for t in range(2)
        ]

    def store_fields(dens, mine):
        for step in range(STEPS):
            field_a, field_b = mixed(dens[step][:, 0:ROWS], dens[step][:, ROWS:])
            field[step, :, 0:ROWS] = field_a
            field[step, :, ROWS:] = field_b
        for t, part in enumerate(mixed(*mine)):
            for y in range(4):
                field_ref[y, :, t * NX : (t + 1) * NX] = part[y * ZDEV : (y + 1) * ZDEV, :]

    def upper(rows):
        return jnp.floor(rows * (1.0 / 256.0))

    def lower(rows):
        return rows - 256.0 * upper(rows)

    @pl.when(jnp.logical_not(many))
    def _():
        store_fields(whole(count_lo), own(lambda rows: rows))

    @pl.when(many)
    def _():
        for i in range(0, STEPS * half, 64):
            count_lo[i : i + 64, :] = lower(count[i : i + 64, :]).astype(BF16)
            count_hi[i : i + 64, :] = upper(count[i : i + 64, :]).astype(BF16)
        for step, part in enumerate(whole(count_hi)):
            dens[step] = 256.0 * part
        store_fields(
            [dens[step] + part for step, part in enumerate(whole(count_lo))],
            [256.0 * a + b for a, b in zip(own(upper), own(lower))],
        )

    column = lax.broadcasted_iota(jnp.int32, (256, CHUNK), 0).astype(F32)
    for step in range(STEPS):
        for block in range(0, blocks, 2):
            at = (step * blocks + block) * 8
            read = []
            for which in range(2):
                row, part, low = [
                    jnp.concatenate([own_ref[at + d : at + d + 1, :], own_ref[at + 8 + d : at + 9 + d, :]], axis=1)
                    for d in range(which * 3, which * 3 + 3)
                ]
                picked = jnp.zeros((256, CHUNK), F32)
                for q in range(4):
                    x_at, t_at = (q & 1) * 256, (q >> 1) * ROWS
                    picked += jnp.dot(
                        field[step, x_at : x_at + 256, t_at : t_at + ROWS],
                        one_hot(jnp.where(part == q + 1.0, row, -1.0), ROWS),
                        preferred_element_type=F32,
                    )
                read.append(jnp.sum(jnp.where(column == low, picked, 0.0), axis=0, keepdims=True))
            got = read[1] - read[0]
            to = step * blocks + block
            values[to : to + 1, :] = got[:, 0:SLOTS]
            values[to + 1 : to + 2, :] = got[:, SLOTS:]
    lists = values[...].astype(BF16)
    for j in range(SLABS):
        value_ref[j] = lists


def change_kernel(value_ref, slot_ref, spare_ref, change_ref):
    lines = slot_ref.shape[1]
    blocks = lines * 128 // BLOCK
    other = spare_ref[STEPS * lines : STEPS * lines + 8, :] > 0.0
    for step in range(STEPS):
        for block in range(blocks):
            change = jnp.zeros((8, 128), F32)
            at = step * blocks + block
            for which in range(2):
                slot = slot_ref[which * STEPS + step, block * 8 : block * 8 + 8, :]
                rank = slot & (SLOTS - 1)
                home = slot >> 7
                total = jnp.zeros((8, 128), F32)
                for j in range(SLABS):
                    line = jnp.broadcast_to(value_ref[j, at : at + 1, :].astype(F32), (8, 128))
                    total = jnp.where(home == j, jnp.take_along_axis(line, rank, axis=1), total)
                change = change + total
            row = step * lines + block * 8
            change = jnp.where(other, spare_ref[row : row + 8, :], change)
            for i in range(8):
                lanes = slice((block * 8 + i) * 128, (block * 8 + i + 1) * 128)
                change_ref[step : step + 1, lanes] = change[i : i + 1, :]


VMEM = pl.BlockSpec(memory_space=pltpu.VMEM)
SMEM = pl.BlockSpec(memory_space=pltpu.SMEM)
ROOM = pltpu.CompilerParams(vmem_limit_bytes=24 * 2**20)


def shape(dims, dtype):
    return jax.ShapeDtypeStruct(dims, dtype)


def local(cells_start, moves, accepted, bead_types):
    beads = cells_start.shape[0]
    chunks = beads // CHUNK
    blocks = beads // BLOCK
    slab = lax.axis_index("grid").astype(jnp.int32).reshape(1)
    place = lax.axis_index("mol").astype(jnp.int32).reshape(1)
    scale = NX * NY * ZDEV * SLABS / (beads * lax.axis_size("mol"))
    msg, code = pl.pallas_call(
        bucket_kernel,
        out_shape=(shape((SLABS, 32, SLOTS), BF16), shape((SETS, beads), jnp.int32)),
        in_specs=[SMEM] + [VMEM] * 4,
        out_specs=(VMEM, VMEM),
        compiler_params=ROOM,
        scratch_shapes=[
            pltpu.VMEM((SETS, beads), F32),
            pltpu.VMEM((4 * SETS, beads), F32),
            pltpu.VMEM((SETS, beads), F32),
            pltpu.VMEM((SETS, beads), F32),
            pltpu.VMEM((STEPS * chunks * 16, CHUNK), BF16),
            pltpu.VMEM((STEPS * chunks * 16, CHUNK + 128), F32),
        ],
        name="bucket",
    )(slab, cells_start.reshape(1, beads), jnp.moveaxis(moves, 1, 0), accepted, bead_types.reshape(1, beads))
    msg = lax.all_to_all(msg, "mol", split_axis=0, concat_axis=0, tiled=True)
    own, slot, table = pl.pallas_call(
        functools.partial(rank_kernel, scale),
        out_shape=(
            shape((STEPS * blocks * 8 + 8, SLOTS), F32),
            shape((SETS, beads // 128, 128), jnp.int32),
            shape((NX, NX), BF16),
        ),
        in_specs=[SMEM, VMEM],
        out_specs=(VMEM, VMEM, VMEM),
        compiler_params=ROOM,
        scratch_shapes=[
            pltpu.VMEM((SETS, beads), F32),
            pltpu.VMEM((3 * SETS, beads), F32),
            pltpu.VMEM((STEPS * chunks * 16, CHUNK), BF16),
            pltpu.VMEM((STEPS * chunks * 16, CHUNK + 128), F32),
        ],
        name="ranks",
    )(slab, code)
    field, value, crowd = pl.pallas_call(
        field_kernel,
        out_shape=(
            shape((4, ZDEV, 2 * NX), BF16),
            shape((SLABS, STEPS * blocks, SLOTS), BF16),
            shape((1,), jnp.int32),
        ),
        in_specs=[SMEM] + [VMEM] * 3,
        out_specs=(VMEM, VMEM, SMEM),
        compiler_params=ROOM,
        scratch_shapes=[
            pltpu.VMEM((2, 32, SLABS * ROOMS), F32),
            pltpu.VMEM((STEPS * ROWS * 2, NX), F32),
            pltpu.VMEM((STEPS * ROWS * 2, NX), BF16),
            pltpu.VMEM((STEPS * ROWS * 2, NX), BF16),
            pltpu.VMEM((STEPS, NX, ROWS * 2), F32),
            pltpu.VMEM((STEPS, NX, ROWS * 2), BF16),
            pltpu.VMEM((STEPS * blocks, SLOTS), F32),
        ],
        name="fields",
    )(place, msg, own, table)
    value = lax.all_to_all(value, "grid", split_axis=0, concat_axis=0, tiled=True)


    def general(spare, field, *arguments):
        change, field = any_spread(*arguments)
        return jnp.concatenate([change.reshape(-1, SLOTS), jnp.ones((8, SLOTS), F32)], axis=0), field

    value, own = lax.optimization_barrier((value, own))
    spare, field = lax.cond(
        crowd[0] == 1, general, lambda spare, field, *_: (spare, field),
        own, field, cells_start, moves, accepted, bead_types,
    )
    change = pl.pallas_call(
        change_kernel,
        out_shape=shape((STEPS, beads), F32),
        in_specs=[VMEM] * 3,
        out_specs=VMEM,
        compiler_params=ROOM,
        name="changes",
    )(value, slot, spare)
    return change, field


def solution(mesh):
    return jax.shard_map(
        local,
        mesh=mesh,
        in_specs=(P("mol"), P(None, None, "mol"), P(None, "mol"), P("mol")),
        out_specs=(P(None, "mol"), P("mol", "grid", None)),
        check_vma=False,
    )
```

```python
import functools

import jax
import jax.numpy as jnp
from jax import lax
from jax.experimental import pallas as pl
from jax.experimental.pallas import tpu as pltpu
from jax.sharding import PartitionSpec as P

NX = 512
NY = 64
ZDEV = 4
STEPS = 2
SPREAD = 2
SLABS = 16
BANDS = 16
SLOTS = 128
ROOMS = 64
CHUNK = 256
BLOCK = 1024
SETS = 4
ROWS = NY * ZDEV
MARK = 320.0
F32 = jnp.float32
BF16 = jnp.bfloat16
LANES = (((1,), (1,)), ((), ()))


chi_mix = 1.0
kappa_comp = 0.5


def split_up(x, dim, size):
    shape = x.shape
    blocks = x.reshape(*shape[:dim], size, shape[dim] // size, *shape[dim + 1 :])
    return jnp.moveaxis(blocks, dim, 0)


def sum_at_owner(x, axis, dim):
    blocks = split_up(x, dim, lax.axis_size(axis))
    arrived = lax.all_to_all(blocks, axis, split_axis=0, concat_axis=0, tiled=True)
    return arrived.sum(axis=0)


def laid_out(blocks, dim):
    blocks = jnp.moveaxis(blocks, 0, dim)
    shape = blocks.shape
    return blocks.reshape(*shape[:dim], shape[dim] * shape[dim + 1], *shape[dim + 2 :])


def sent_to_all(x, axis):
    copies = jnp.broadcast_to(x, (lax.axis_size(axis), *x.shape))
    return lax.all_to_all(copies, axis, split_axis=0, concat_axis=0, tiled=True)


def collect(x, axis, dim):
    return laid_out(sent_to_all(x, axis), dim)


def of_everyone(x, axis):
    return sent_to_all(x, axis).astype(jnp.float32).sum(axis=0)


def kernel_rows(col_x):
    column = jnp.arange(NX, dtype=jnp.float32)
    distance = jnp.abs(column[None, :] - col_x.astype(jnp.float32)[:, None])
    distance = jnp.minimum(distance, NX - distance)
    weights = jnp.exp(-distance * distance / (2.0 * SPREAD * SPREAD))
    first = jnp.abs(column)
    first = jnp.minimum(first, NX - first)
    total = jnp.sum(jnp.exp(-first * first / (2.0 * SPREAD * SPREAD)))
    return (weights / total).astype(jnp.bfloat16)


def split_cell(cells):
    col_x = cells % NX
    row_y = cells // NX % NY
    plane_z = cells // (NX * NY)
    return (col_x, row_y, plane_z)


def move_cells(cells, shift, planes):
    col_x, row_y, plane_z = split_cell(cells)
    col_x = (col_x + shift[0]) % NX
    row_y = (row_y + shift[1]) % NY
    plane_z = (plane_z + shift[2]) % planes
    return (plane_z * NY + row_y) * NX + col_x


def deposit(positions, bead_types, slab, start, count):
    col_x, row_y, plane_z = split_cell(positions)
    inside = (plane_z // ZDEV == slab) & (row_y >= start) & (row_y < start + count)
    row_id = jnp.where(inside, row_y * ZDEV + plane_z - slab * ZDEV, -1)
    bead_count = positions.shape[0]
    block_size = min(1024, bead_count)
    row_total = count * ZDEV
    targets = lax.broadcasted_iota(jnp.int32, (row_total, block_size), 0)

    def add_block(block_id, total):
        begin = block_id * block_size
        rows_here = lax.dynamic_slice_in_dim(row_id, begin, block_size)
        cols_here = lax.dynamic_slice_in_dim(col_x, begin, block_size)
        types_here = lax.dynamic_slice_in_dim(bead_types, begin, block_size)
        onehot = (rows_here[None, :] == targets).astype(jnp.bfloat16)
        spread_rows = kernel_rows(cols_here)
        zeros_bf = jnp.zeros_like(spread_rows)
        first = jnp.where(types_here[:, None] == 0, spread_rows, zeros_bf)
        second = jnp.where(types_here[:, None] == 1, spread_rows, zeros_bf)
        columns = jnp.concatenate([first, second], axis=1)
        return total + jnp.dot(onehot, columns, preferred_element_type=jnp.float32)

    empty = jnp.zeros((row_total, 2 * NX), jnp.float32)
    total = lax.fori_loop(0, bead_count // block_size, add_block, empty)
    return total.reshape(count, ZDEV, 2 * NX)


def make_field(density):
    phi_a = density[:, :, :NX]
    phi_b = density[:, :, NX:]
    excess = kappa_comp * (phi_a + phi_b - 1.0)
    field_a = chi_mix * phi_b + excess
    field_b = chi_mix * phi_a + excess
    return jnp.concatenate([field_a, field_b], axis=2).astype(jnp.bfloat16)


def make_reader(points, bead_types, z_first, z_span):
    col_x, row_y, plane_z = split_cell(points)
    local_z = plane_z - z_first
    kinds = jnp.broadcast_to(bead_types[None, :], points.shape)
    column_id = kinds * NX + col_x

    def read_beads(carry, piece, start):
        span_rows = piece.shape[0]
        flat_table = piece.reshape(-1)
        valid = (row_y >= 0) & (row_y < span_rows) & (local_z >= 0) & (local_z < z_span)
        flat_index = jnp.where(valid, (row_y * z_span + local_z) * (2 * NX) + column_id, 0)
        picked = jnp.take(flat_table, flat_index).astype(jnp.float32)
        return jnp.where(valid, picked, 0.0)

    return read_beads


def any_spread(cells_start, moves, accepted, bead_types):
    grid_count = lax.axis_size("grid")
    mol_count = lax.axis_size("mol")
    slab = lax.axis_index("grid")
    planes = ZDEV * grid_count
    bead_count = cells_start.shape[0]
    scale = NX * NY * planes / (bead_count * mol_count)
    band_rows = NY // mol_count
    positions = [cells_start]
    proposals = []
    for step in range(STEPS):
        proposed = move_cells(positions[step], moves[step], planes)
        proposals.append(proposed)
        positions.append(jnp.where(accepted[step] == 1, proposed, positions[step]))
    fields = []
    for step in range(STEPS):

        def step_term(start, count, current=positions[step]):
            return deposit(current, bead_types, slab, start, count)

        summed = sum_at_owner(step_term(jnp.int32(0), band_rows * lax.axis_size("mol")), "mol", 0)
        fields.append(make_field(scale * summed))
    changes = []
    for step in range(STEPS):
        points = jnp.stack([positions[step], proposals[step]])
        start_values = jnp.zeros(points.shape, jnp.float32)
        reader = make_reader(points, bead_types, slab * ZDEV, ZDEV)
        partial_values = reader(start_values, collect(fields[step], "mol", 0), jnp.int32(0))
        values = of_everyone(partial_values.astype(jnp.bfloat16), "grid").astype(jnp.float32)
        changes.append(values[1] - values[0])
    return (jnp.stack(changes), fields[STEPS - 1])


def one_hot(row, count, base=0):
    width = row.shape[1]
    tile = jnp.broadcast_to(row, (16, width)).astype(BF16)
    iota = lax.broadcasted_iota(jnp.int32, (16, width), 0).astype(F32)
    one = jnp.ones((16, width), BF16)
    zero = jnp.zeros((16, width), BF16)
    parts = [
        jnp.where(tile == (iota + float(base + first)).astype(BF16), one, zero)
        for first in range(0, count, 16)
    ]
    return jnp.concatenate(parts, axis=0) if len(parts) > 1 else parts[0]


def prefix_matrix():
    rows = lax.broadcasted_iota(jnp.int32, (CHUNK, CHUNK + 128), 0)
    cols = lax.broadcasted_iota(jnp.int32, (CHUNK, CHUNK + 128), 1)
    return jnp.where((rows <= cols) | (cols >= CHUNK), 1.0, 0.0).astype(BF16)


def bucket_kernel(slab_ref, cells_ref, moves_ref, accepted_ref, types_ref, msg_ref, code_ref,
                  slabs, bands, highs, lows, ranked, prefix):
    beads = cells_ref.shape[1]
    chunks = beads // CHUNK
    slab = slab_ref[0]
    kind = types_ref[...] << 21

    def moved(cell, step):
        col_x = (cell + moves_ref[0, step : step + 1, :]) & (NX - 1)
        row_y = ((cell >> 9) + moves_ref[1, step : step + 1, :]) & (NY - 1)
        plane = ((cell >> 15) + moves_ref[2, step : step + 1, :]) & (ZDEV * SLABS - 1)
        return col_x | (row_y << 9) | (plane << 15)

    start = cells_ref[...]
    first = moved(start, 0)
    after = jnp.where(accepted_ref[0:1, :] == 1, first, start)
    second = moved(after, 1)
    code_ref[0:1, :] = start | kind
    code_ref[1:2, :] = after | kind
    code_ref[2:3, :] = first | kind
    code_ref[3:4, :] = second | kind
    c = code_ref[...]
    slabs[...] = ((c >> 17) & 15).astype(F32)
    band = (c >> 11) & 15
    inside = ((c >> 17) & 15) == slab
    bands[0:SETS, :] = band.astype(F32)
    bands[SETS : 2 * SETS, :] = jnp.where(inside, band, -64).astype(F32)
    bands[2 * SETS : 3 * SETS, :] = jnp.where(inside, band & 7, -64).astype(F32)
    bands[3 * SETS : 4 * SETS, :] = ((band >> 3) * ROOMS).astype(F32)
    highs[...] = (((c >> 7) & 3) * 32 + (c >> 21) * 16 + ((c >> 9) & 3) * 4 + ((c >> 15) & 3) + 1).astype(F32)
    lows[...] = (c & 127).astype(F32)
    counts = jnp.zeros((SETS * 16, 48), F32)
    upper = lax.broadcasted_iota(jnp.int32, (16, CHUNK), 0) >= 8
    own_row = (lax.broadcasted_iota(jnp.int32, (16, CHUNK), 0) & 7).astype(F32).astype(BF16)
    zero = jnp.zeros((16, CHUNK), BF16)
    for k in range(chunks):
        lanes = slice(k * CHUNK, (k + 1) * CHUNK)
        alone = [one_hot(slabs[s : s + 1, lanes], 16) for s in range(SETS)]
        either = [jnp.maximum(alone[s], alone[STEPS + s]) for s in range(STEPS)]
        of_slab = jnp.concatenate(alone[0:STEPS] + either, axis=0)
        kinds = [one_hot(bands[s : s + 1, lanes], 16) for s in range(STEPS)]
        kinds.append(one_hot(jnp.full((1, CHUNK), float(k * CHUNK // BLOCK), F32), 16))
        counts += lax.dot_general(of_slab, jnp.concatenate(kinds, axis=0), LANES, preferred_element_type=F32)
        for s in range(STEPS):
            at = (s * chunks + k) * 16
            ranked[at : at + 16, :] = one_hot(bands[SETS + s : SETS + s + 1, lanes], 16)
    set_of = lax.broadcasted_iota(jnp.int32, counts.shape, 0) // 16
    kind_of = lax.broadcasted_iota(jnp.int32, counts.shape, 1) // 16
    listed = (kind_of == STEPS) & (set_of >= STEPS)
    limit = jnp.where(listed, float(SLOTS), jnp.where(set_of == kind_of, float(ROOMS), float(beads)))
    crowded = jnp.max(counts - limit) > 0.0
    prefix[...] = jnp.dot(ranked[...], prefix_matrix(), preferred_element_type=F32)
    out = []
    for s in range(STEPS):
        carry = jnp.zeros((16, 128), F32)
        lists = jnp.zeros((16, SLOTS), F32)
        for k in range(chunks):
            at = (s * chunks + k) * 16
            lanes = slice(k * CHUNK, (k + 1) * CHUNK)
            ahead = prefix[at : at + 16, 0:CHUNK] + jnp.concatenate([carry, carry], axis=1)
            carry = carry + prefix[at : at + 16, CHUNK : CHUNK + 128]
            rank = jnp.sum(ranked[at : at + 16, :].astype(F32) * ahead, axis=0, keepdims=True) - 1.0
            lane = jnp.where(rank >= 0.0, rank + bands[3 * SETS + s : 3 * SETS + s + 1, lanes], -1.0)
            low = jnp.broadcast_to(lows[s : s + 1, lanes], (16, CHUNK))
            high = jnp.broadcast_to(highs[s : s + 1, lanes], (16, CHUNK))
            row = jnp.broadcast_to(bands[2 * SETS + s : 2 * SETS + s + 1, lanes], (16, CHUNK)).astype(BF16)
            left = jnp.where(row == own_row, jnp.where(upper, low, high).astype(BF16), zero)
            lists += lax.dot_general(left, one_hot(lane, SLOTS), LANES, preferred_element_type=F32)
        out.append(lists)
    corner = (lax.broadcasted_iota(jnp.int32, (16, SLOTS), 0) == 0) & (
        lax.broadcasted_iota(jnp.int32, (16, SLOTS), 1) == 0
    )
    out[0] = jnp.where(corner & crowded, MARK, out[0])
    message = jnp.concatenate(out, axis=0).astype(BF16)
    for j in range(SLABS):
        msg_ref[j] = message


def rank_kernel(scale, slab_ref, code_ref, own_ref, slot_ref, table_ref, slabs, digits, ranked, prefix):
    column = lax.broadcasted_iota(jnp.int32, (8, NX), 1)
    distance = jnp.minimum(column, NX - column).astype(F32)
    weights = jnp.exp(-distance * distance / (2.0 * SPREAD * SPREAD))
    first = (weights / jnp.sum(weights[0:1, :], axis=1, keepdims=True))[0:1, :]
    turned = pltpu.roll(jnp.broadcast_to(first, (NX, NX)), 0, 1, stride=1, stride_axis=0)
    table_ref[...] = turned.astype(BF16) * jnp.full((NX, NX), scale, BF16)
    beads = code_ref.shape[1]
    chunks = beads // CHUNK
    c = code_ref[...]
    home = (c >> 17) & 15
    slabs[...] = home.astype(F32)
    digits[0:SETS, :] = (((c >> 9) & 63) * 4 + ((c >> 15) & 3)).astype(F32)
    digits[SETS : 2 * SETS, :] = jnp.where(home == slab_ref[0], (c >> 21) * 2 + ((c >> 8) & 1) + 1, 0).astype(F32)
    digits[2 * SETS : 3 * SETS, :] = (c & 255).astype(F32)
    here = slab_ref[0].astype(F32)
    for s in range(STEPS):
        for k in range(chunks):
            at = (s * chunks + k) * 16
            lanes = slice(k * CHUNK, (k + 1) * CHUNK)
            ranked[at : at + 16, :] = jnp.maximum(
                one_hot(slabs[s : s + 1, lanes], 16), one_hot(slabs[STEPS + s : STEPS + s + 1, lanes], 16)
            )
    prefix[...] = jnp.dot(ranked[...], prefix_matrix(), preferred_element_type=F32)
    sixteen = lax.broadcasted_iota(jnp.int32, (16, CHUNK), 0).astype(F32)
    eight = lax.broadcasted_iota(jnp.int32, (8, CHUNK), 0)
    for s in range(STEPS):
        for block in range(beads // BLOCK):
            carry = jnp.zeros((16, 128), F32)
            lists = jnp.zeros((8, SLOTS), F32)
            for k in range(block * BLOCK // CHUNK, (block + 1) * BLOCK // CHUNK):
                at = (s * chunks + k) * 16
                lanes = slice(k * CHUNK, (k + 1) * CHUNK)
                ahead = prefix[at : at + 16, 0:CHUNK] + jnp.concatenate([carry, carry], axis=1)
                carry = carry + prefix[at : at + 16, CHUNK : CHUNK + 128]
                homes, ranks = [], []
                for p in (s, STEPS + s):
                    homes.append(slabs[p : p + 1, lanes])
                    mine = jnp.where(sixteen == jnp.broadcast_to(homes[-1], (16, CHUNK)), ahead, 0.0)
                    ranks.append(jnp.sum(mine, axis=0, keepdims=True) - 1.0)
                first = homes[0] * float(SLOTS) + ranks[0]
                second = jnp.where(homes[0] == homes[1], float(-SLOTS), homes[1] * float(SLOTS) + ranks[1])
                for p, slot in ((s, first.astype(jnp.int32)), (STEPS + s, second.astype(jnp.int32))):
                    for i in range(CHUNK // 128):
                        line = k * CHUNK // 128 + i
                        slot_ref[p, line : line + 1, :] = slot[:, i * 128 : (i + 1) * 128]
                held = jnp.where(homes[0] == here, ranks[0], jnp.where(homes[1] == here, ranks[1], -1.0))
                left = jnp.zeros((8, CHUNK), F32)
                for d in range(6):
                    row = d % 3 * SETS + d // 3 * STEPS + s
                    left = jnp.where(eight == d, jnp.broadcast_to(digits[row : row + 1, lanes], (8, CHUNK)), left)
                lists += lax.dot_general(left.astype(BF16), one_hot(held, SLOTS), LANES, preferred_element_type=F32)
            at = (s * (beads // BLOCK) + block) * 8
            own_ref[at : at + 8, :] = lists
    own_ref[STEPS * chunks * CHUNK // 128 :, :] = jnp.zeros((8, SLOTS), F32)


def field_kernel(place_ref, msg_ref, own_ref, table_ref, field_ref, value_ref, crowd_ref,
                 slots, count, count_lo, count_hi, dens, field, values):
    blocks = (own_ref.shape[0] - 8) // (8 * STEPS)
    half = ROWS * 2
    marks = msg_ref[0, 0:1, :].astype(F32)
    for j in range(1, SLABS):
        marks = jnp.maximum(marks, msg_ref[j, 0:1, :].astype(F32))
    crowd_ref[0] = (jnp.max(marks) >= MARK).astype(jnp.int32)
    most = jnp.zeros((8, SLOTS), F32)
    left_half = lax.broadcasted_iota(jnp.int32, (32, SLOTS), 1) < ROOMS
    for j in range(0, SLABS, 2):
        even, odd = msg_ref[j].astype(F32), msg_ref[j + 1].astype(F32)
        lanes = slice(j // 2 * SLOTS, (j // 2 + 1) * SLOTS)
        slots[0, :, lanes] = jnp.where(left_half, even, pltpu.roll(odd, ROOMS, 1))
        slots[1, :, lanes] = jnp.where(left_half, pltpu.roll(even, ROOMS, 1), odd)
    for step in range(STEPS):
        for band in range(BANDS):
            hist = jnp.zeros((128, 128), F32)
            at = step * 16 + band % 8
            for k in range(0, slots.shape[2], CHUNK):
                hist += lax.dot_general(
                    one_hot(slots[band // 8, at : at + 1, k : k + CHUNK], 128, 1),
                    one_hot(slots[band // 8, at + 8 : at + 9, k : k + CHUNK], 128),
                    LANES,
                    preferred_element_type=F32,
                )
            for q in range(4):
                for t in range(2):
                    at = step * half + t * ROWS + band * 16
                    part = hist[q * 32 + t * 16 : q * 32 + t * 16 + 16, :]
                    count[at : at + 16, q * 128 : (q + 1) * 128] = part
                    count_lo[at : at + 16, q * 128 : (q + 1) * 128] = part.astype(BF16)
                    most = jnp.maximum(most, jnp.maximum(part[0:8, :], part[8:16, :]))
    many = jnp.max(most) > 256.0

    def mixed(phi_a, phi_b):
        excess = kappa_comp * (phi_a + phi_b - 1.0)
        return (chi_mix * phi_b + excess).astype(BF16), (chi_mix * phi_a + excess).astype(BF16)

    def whole(counts):
        return [
            lax.dot_general(table_ref[...], counts[step * half : (step + 1) * half, :], LANES, preferred_element_type=F32)
            for step in range(STEPS)
        ]

    def own(digit):
        at = (STEPS - 1) * half + place_ref[0] * 16
        return [
            jnp.dot(
                digit(count[pl.ds(pl.multiple_of(at + t * ROWS, 16), 16), :]).astype(BF16),
                table_ref[...],
                preferred_element_type=F32,
            )
            for t in range(2)
        ]

    def store_fields(dens, mine):
        for step in range(STEPS):
            field_a, field_b = mixed(dens[step][:, 0:ROWS], dens[step][:, ROWS:])
            field[step, :, 0:ROWS] = field_a
            field[step, :, ROWS:] = field_b
        for t, part in enumerate(mixed(*mine)):
            for y in range(4):
                field_ref[y, :, t * NX : (t + 1) * NX] = part[y * ZDEV : (y + 1) * ZDEV, :]

    def upper(rows):
        return jnp.floor(rows * (1.0 / 256.0))

    def lower(rows):
        return rows - 256.0 * upper(rows)

    @pl.when(jnp.logical_not(many))
    def _():
        store_fields(whole(count_lo), own(lambda rows: rows))

    @pl.when(many)
    def _():
        for i in range(0, STEPS * half, 64):
            count_lo[i : i + 64, :] = lower(count[i : i + 64, :]).astype(BF16)
            count_hi[i : i + 64, :] = upper(count[i : i + 64, :]).astype(BF16)
        for step, part in enumerate(whole(count_hi)):
            dens[step] = 256.0 * part
        store_fields(
            [dens[step] + part for step, part in enumerate(whole(count_lo))],
            [256.0 * a + b for a, b in zip(own(upper), own(lower))],
        )

    column = lax.broadcasted_iota(jnp.int32, (256, CHUNK), 0).astype(F32)
    for step in range(STEPS):
        for block in range(0, blocks, 2):
            at = (step * blocks + block) * 8
            read = []
            for which in range(2):
                row, part, low = [
                    jnp.concatenate([own_ref[at + d : at + d + 1, :], own_ref[at + 8 + d : at + 9 + d, :]], axis=1)
                    for d in range(which * 3, which * 3 + 3)
                ]
                picked = jnp.zeros((256, CHUNK), F32)
                for q in range(4):
                    x_at, t_at = (q & 1) * 256, (q >> 1) * ROWS
                    picked += jnp.dot(
                        field[step, x_at : x_at + 256, t_at : t_at + ROWS],
                        one_hot(jnp.where(part == q + 1.0, row, -1.0), ROWS),
                        preferred_element_type=F32,
                    )
                read.append(jnp.where(column == low, picked, 0.0))
            got = jnp.sum(read[1] - read[0], axis=0, keepdims=True)
            to = step * blocks + block
            values[to : to + 1, :] = got[:, 0:SLOTS]
            values[to + 1 : to + 2, :] = got[:, SLOTS:]
    lists = values[...].astype(BF16)
    for j in range(SLABS):
        value_ref[j] = lists


def change_kernel(value_ref, slot_ref, spare_ref, change_ref):
    lines = slot_ref.shape[1]
    blocks = lines * 128 // BLOCK
    other = spare_ref[STEPS * lines : STEPS * lines + 8, :] > 0.0
    for step in range(STEPS):
        for block in range(blocks):
            change = jnp.zeros((8, 128), F32)
            at = step * blocks + block
            for which in range(2):
                slot = slot_ref[which * STEPS + step, block * 8 : block * 8 + 8, :]
                rank = slot & (SLOTS - 1)
                home = slot >> 7
                total = jnp.zeros((8, 128), F32)
                for j in range(SLABS):
                    line = jnp.broadcast_to(value_ref[j, at : at + 1, :].astype(F32), (8, 128))
                    total = jnp.where(home == j, jnp.take_along_axis(line, rank, axis=1), total)
                change = change + total
            row = step * lines + block * 8
            change = jnp.where(other, spare_ref[row : row + 8, :], change)
            for i in range(8):
                lanes = slice((block * 8 + i) * 128, (block * 8 + i + 1) * 128)
                change_ref[step : step + 1, lanes] = change[i : i + 1, :]


VMEM = pl.BlockSpec(memory_space=pltpu.VMEM)
SMEM = pl.BlockSpec(memory_space=pltpu.SMEM)
ROOM = pltpu.CompilerParams(vmem_limit_bytes=24 * 2**20)


def shape(dims, dtype):
    return jax.ShapeDtypeStruct(dims, dtype)


def local(cells_start, moves, accepted, bead_types):
    beads = cells_start.shape[0]
    chunks = beads // CHUNK
    blocks = beads // BLOCK
    slab = lax.axis_index("grid").astype(jnp.int32).reshape(1)
    place = lax.axis_index("mol").astype(jnp.int32).reshape(1)
    scale = NX * NY * ZDEV * SLABS / (beads * lax.axis_size("mol"))
    msg, code = pl.pallas_call(
        bucket_kernel,
        out_shape=(shape((SLABS, 32, SLOTS), BF16), shape((SETS, beads), jnp.int32)),
        in_specs=[SMEM] + [VMEM] * 4,
        out_specs=(VMEM, VMEM),
        compiler_params=ROOM,
        scratch_shapes=[
            pltpu.VMEM((SETS, beads), F32),
            pltpu.VMEM((4 * SETS, beads), F32),
            pltpu.VMEM((SETS, beads), F32),
            pltpu.VMEM((SETS, beads), F32),
            pltpu.VMEM((STEPS * chunks * 16, CHUNK), BF16),
            pltpu.VMEM((STEPS * chunks * 16, CHUNK + 128), F32),
        ],
        name="bucket",
    )(slab, cells_start.reshape(1, beads), jnp.moveaxis(moves, 1, 0), accepted, bead_types.reshape(1, beads))
    msg = lax.all_to_all(msg, "mol", split_axis=0, concat_axis=0, tiled=True)
    own, slot, table = pl.pallas_call(
        functools.partial(rank_kernel, scale),
        out_shape=(
            shape((STEPS * blocks * 8 + 8, SLOTS), F32),
            shape((SETS, beads // 128, 128), jnp.int32),
            shape((NX, NX), BF16),
        ),
        in_specs=[SMEM, VMEM],
        out_specs=(VMEM, VMEM, VMEM),
        compiler_params=ROOM,
        scratch_shapes=[
            pltpu.VMEM((SETS, beads), F32),
            pltpu.VMEM((3 * SETS, beads), F32),
            pltpu.VMEM((STEPS * chunks * 16, CHUNK), BF16),
            pltpu.VMEM((STEPS * chunks * 16, CHUNK + 128), F32),
        ],
        name="ranks",
    )(slab, code)
    field, value, crowd = pl.pallas_call(
        field_kernel,
        out_shape=(
            shape((4, ZDEV, 2 * NX), BF16),
            shape((SLABS, STEPS * blocks, SLOTS), BF16),
            shape((1,), jnp.int32),
        ),
        in_specs=[SMEM] + [VMEM] * 3,
        out_specs=(VMEM, VMEM, SMEM),
        compiler_params=ROOM,
        scratch_shapes=[
            pltpu.VMEM((2, 32, SLABS * ROOMS), F32),
            pltpu.VMEM((STEPS * ROWS * 2, NX), F32),
            pltpu.VMEM((STEPS * ROWS * 2, NX), BF16),
            pltpu.VMEM((STEPS * ROWS * 2, NX), BF16),
            pltpu.VMEM((STEPS, NX, ROWS * 2), F32),
            pltpu.VMEM((STEPS, NX, ROWS * 2), BF16),
            pltpu.VMEM((STEPS * blocks, SLOTS), F32),
        ],
        name="fields",
    )(place, msg, own, table)
    value = lax.all_to_all(value, "grid", split_axis=0, concat_axis=0, tiled=True)


    def general(spare, field, *arguments):
        change, field = any_spread(*arguments)
        return jnp.concatenate([change.reshape(-1, SLOTS), jnp.ones((8, SLOTS), F32)], axis=0), field

    value, own = lax.optimization_barrier((value, own))
    spare, field = lax.cond(
        crowd[0] == 1, general, lambda spare, field, *_: (spare, field),
        own, field, cells_start, moves, accepted, bead_types,
    )
    change = pl.pallas_call(
        change_kernel,
        out_shape=shape((STEPS, beads), F32),
        in_specs=[VMEM] * 3,
        out_specs=VMEM,
        compiler_params=ROOM,
        name="changes",
    )(value, slot, spare)
    return change, field


def solution(mesh):
    return jax.shard_map(
        local,
        mesh=mesh,
        in_specs=(P("mol"), P(None, None, "mol"), P(None, "mol"), P("mol")),
        out_specs=(P(None, "mol"), P("mol", "grid", None)),
        check_vma=False,
    )
```
